256 devices in a mesh: blk: 8 (over x, core), grp: 32 (over z, y).
Axes of the slice: x: 4, y: 4, z: 8, core: 2. Of those that a mesh axis runs over, the one named last changes fastest.
Arguments:
- features: float32 [393216, 256], P(('blk', 'grp')), may hold values from -6 to 6
- initial: bfloat16 [393216, 256], P(('blk', 'grp')), may hold values from -6 to 6
- history: bfloat16 [393216, 256], P(('blk', 'grp')), may hold values from -6 to 6
- weight: bfloat16 [256, 256], replicated, may hold values from -0.375 to 0.375
- column_ids: int32 [3072, 16], P(('blk', 'grp')), may hold values from 0 to 51, as said below
- block_values: bfloat16 [3072, 16, 128, 128], P(('blk', 'grp')), may hold values from -0.125 to 0.125
- group_table: int32 [8, 32, 32], P('blk'), may hold values from 0 to 11
- loop_table: int32 [32, 8, 8], P('grp'), may hold values from 0 to 11
Outputs:
- refreshed: float32 [393216, 256], P(('blk', 'grp'))
- inbox: float32 [393216, 256], P(('blk', 'grp'))
The draws below stay inside these ranges and needn't reach their ends.
Inputs may be any that keep to these rules, and one draw needn't show every extreme that they name: `column_ids`: among the 16 entries of the 12 row tiles of one device, every slot from 0 to 12 + 32 + 8 - 1 appears at least once.
All inputs are finite; a program needn't handle non-finite values.
Results may differ from the reference program's by a relative error of at most 0.004.
Values may be sent and summed in bfloat16 or wider, within the bound.
A program may use at most 128 MiB of HBM per device.

```python
import math
import jax
import jax.numpy as jnp
import numpy as np
from jax import lax

H = 256
TILE = 128
K = 16
BLK_DEV = 12
TILES = 3072
NODES = 393216
N_BLK = 8
N_GRP = 32


def draw_column_ids(key, part):
    slots = BLK_DEV + N_GRP + N_BLK
    count = BLK_DEV * K
    device_count = N_BLK * N_GRP
    device_keys = jax.random.split(jax.random.fold_in(key, 7), device_count)

    def one_device(device_key):
        first_key, second_key = jax.random.split(device_key)
        extra = jax.random.randint(first_key, (count - slots,), 0, slots).astype(jnp.int32)
        base = jnp.concatenate([jnp.arange(slots, dtype=jnp.int32), extra])
        return jax.random.permutation(second_key, base).reshape(BLK_DEV, K)
    return jax.vmap(one_device)(device_keys).reshape(device_count * BLK_DEV, K).astype(jnp.int32)


def plant(result, stream_key, least, high):
    spot = [jax.random.randint(jax.random.fold_in(stream_key, axis), (), 0, length) for axis, length in enumerate(result.shape)]
    main_axis = result.shape.index(max(result.shape))
    next_to = spot[:main_axis] + [(spot[main_axis] + 1) % result.shape[main_axis]] + spot[main_axis + 1:]
    return result.at[tuple(spot)].set(least).at[tuple(next_to)].set(high)


def steps_of(own_key, dims, pieces, low, high):
    gain, own = 1.0, jax.random.fold_in(own_key, 6)
    for dim, shards_of in pieces:
        draws = jnp.exp(jax.random.uniform(jax.random.fold_in(own, dim), (shards_of,), jnp.float32, low / len(pieces), high / len(pieces)))
        gain = gain * jnp.repeat(draws, dims[dim] // shards_of).reshape([-1 if axis == dim else 1 for axis in range(len(dims))])
    return gain


def cumulative_ranks(number_of, skew):
    portions = [(1 << 20) // math.isqrt(rank ** skew) + 1 for rank in range(1, number_of + 1)]
    scale = 1 + sum(portions) // (1 << 30)
    return np.cumsum(np.array([max(1, weight // scale) for weight in portions]))


def skewed_ids(stream_key, extent, number_of, slope):
    grid = cumulative_ranks(number_of, slope)
    pick = jax.random.randint(jax.random.fold_in(stream_key, 1), extent, 0, int(grid[number_of - 1]))
    rank = jnp.searchsorted(jnp.asarray(grid, jnp.int32), pick, side="right")
    return jax.random.permutation(jax.random.fold_in(stream_key, 2), number_of)[rank].astype(jnp.int32)


def centred(key, shape, spread, limit, shards=(), kind=jnp.bfloat16):
    array = spread * jax.random.normal(key, shape, jnp.float32)
    if shards:
        array = array * steps_of(key, shape, shards, -0.22, 0.18)
    return jnp.clip(array, -limit, limit).astype(kind)


def setup_inputs(seed: int = 0) -> dict:
    seeds = jax.random.split(jax.random.key(seed), 9)
    features = centred(seeds[0], (NODES, H), 1.0, 6.0, ((0, 256),), jnp.float32)
    initial = centred(seeds[1], (NODES, H), 1.0, 6.0, ((0, 256),))
    history = centred(seeds[2], (NODES, H), 1.0, 6.0, ((0, 256),))
    weight = centred(seeds[3], (H, H), H ** -0.5, 0.375)
    column_ids = draw_column_ids(jax.random.fold_in(seeds[8], 71), 0)
    block_values = centred(seeds[5], (TILES, K, TILE, TILE), (TILE * K) ** -0.5, 0.125, ((0, 256),))
    group_table = plant(skewed_ids(seeds[6], (N_BLK, N_GRP, N_GRP), BLK_DEV, 2), jax.random.fold_in(seeds[6], 3), 0, BLK_DEV - 1).astype(jnp.int32)
    loop_table = plant(skewed_ids(seeds[7], (N_GRP, N_BLK, N_BLK), BLK_DEV, 2), jax.random.fold_in(seeds[7], 3), 0, BLK_DEV - 1).astype(jnp.int32)
    return {"features": features, "initial": initial, "history": history, "weight": weight, "column_ids": column_ids, "block_values": block_values, "group_table": group_table, "loop_table": loop_table}


teleport = 0.1
mapping_share = 0.5


def reference(features, initial, history, weight, column_ids, block_values, group_table, loop_table):
    device_count = N_BLK * N_GRP
    slots = BLK_DEV + N_GRP + N_BLK
    fresh_blocks = features.astype(jnp.bfloat16).reshape(device_count, BLK_DEV, TILE, H)
    stale_blocks = history.reshape(device_count, BLK_DEV, TILE, H)
    start_blocks = initial.reshape(device_count, BLK_DEV, TILE, H)
    columns = column_ids.reshape(device_count, BLK_DEV, K)
    values = block_values.reshape(device_count, BLK_DEV, K, TILE, TILE)
    group_range = jnp.arange(N_GRP, dtype=jnp.int32)
    loop_range = jnp.arange(N_BLK, dtype=jnp.int32)
    slot_range = jnp.arange(slots, dtype=jnp.int32)

    def owners_of(device):
        loop_pos = device // N_GRP
        group_pos = device % N_GRP
        group_owner = loop_pos * N_GRP + group_range
        loop_owner = loop_range * N_GRP + group_pos
        group_block = group_table[loop_pos, :, group_pos]
        loop_block = loop_table[group_pos, :, loop_pos]
        owner = jnp.concatenate([group_owner, loop_owner]).astype(jnp.int32)
        block = jnp.concatenate([group_block, loop_block]).astype(jnp.int32)
        return owner, block

    def one_device(device):
        owner, block = owners_of(device)
        pulled = stale_blocks[owner, block]
        sources = jnp.concatenate([fresh_blocks[device], pulled], axis=0)
        column_rows = columns[device]
        picked = sources[column_rows].astype(jnp.float32)
        tile_values = values[device].astype(jnp.float32)
        gathered = jnp.einsum('tkij,tkjh->tih', tile_values, picked)
        start = start_blocks[device].astype(jnp.float32)
        mixed = ((1.0 - teleport) * gathered + teleport * start).astype(jnp.bfloat16).reshape(BLK_DEV * TILE, H)
        product = jnp.dot(mixed, weight, preferred_element_type=jnp.float32)
        refreshed = jax.nn.relu((1.0 - mapping_share) * mixed.astype(jnp.float32) + mapping_share * product)
        outgoing = refreshed.astype(jnp.bfloat16).reshape(BLK_DEV, TILE, H).astype(jnp.float32)
        each = jnp.einsum('tkij,tih->tkjh', tile_values, outgoing)
        selector = (column_rows[:, :, None] == slot_range[None, None, :]).astype(jnp.float32)
        messages = jnp.einsum('tks,tkjh->sjh', selector, each, precision=lax.Precision.HIGHEST)
        return refreshed, messages[BLK_DEV:].astype(jnp.bfloat16)

    device_ids = jnp.arange(device_count, dtype=jnp.int32)
    refreshed, messages = lax.map(one_device, device_ids)
    owner, block = jax.vmap(owners_of)(device_ids)
    targets = (owner * BLK_DEV + block).reshape(-1).astype(jnp.int32)
    inbox = jnp.zeros((device_count * BLK_DEV, TILE, H), jnp.float32)
    inbox = inbox.at[targets].add(messages.reshape(-1, TILE, H).astype(jnp.float32))
    return refreshed.reshape(NODES, H), inbox.reshape(NODES, H)
```

```python
import jax
import jax.numpy as jnp
from jax import lax
from jax.experimental import pallas as pl
from jax.experimental.pallas import tpu as pltpu
from jax.sharding import PartitionSpec as P

MESH = pl.DeviceIdType.MESH
teleport = 0.1
mapping_share = 0.5

TILES, ENTRIES, EDGE, HIDDEN = 12, 16, 128, 256
N_Z, N_Y, N_X, N_CORE = 8, 4, 4, 2
N_GRP, N_BLK = N_Z * N_Y, N_X * N_CORE
N_FAR = N_GRP + N_BLK
CHUNK = 4
OWN_CHUNKS, LOOP_CHUNKS, GROUP_CHUNKS = TILES // CHUNK, N_BLK // CHUNK, N_GRP // CHUNK
ROWS = TILES * EDGE
NONE = TILES * ENTRIES


def far_first(k, n):
    return lax.rem(n // 2 + (1 - 2 * lax.rem(k, 2)) * lax.div(k + 1, 2) + n, n)


def kernel(
    feat_h, init_h, hist_h, w_ref, ids_ref, val_h, gt_ref, lt_ref,
    refreshed_h, inbox_h,
    hist_v, feat_v, init_v, own_v, val_v, chain_v, turned_v, adj_v, send_v, pull_v, push_v,
    gath_v, out_v, left_v, box_v, last_v, prev_v, last_s, prev_s,
    in_sem, tab_sem, send_sem, recv_sem, send2_sem, recv2_sem, res_sem,
):
    f32, bf16 = jnp.float32, jnp.bfloat16
    g, b = lax.axis_index("grp"), lax.axis_index("blk")
    z, y = lax.div(g, N_Y), lax.rem(g, N_Y)
    x, core = lax.div(b, N_CORE), lax.rem(b, N_CORE)

    def group_at(i, sign):
        dz, dy = far_first(lax.div(i, N_Y), N_Z), far_first(lax.rem(i, N_Y), N_Y)
        return lax.rem(z + sign * dz + N_Z, N_Z) * N_Y + lax.rem(y + sign * dy + N_Y, N_Y)

    def loop_at(i, sign):
        dx, dc = far_first(lax.div(i, N_CORE), N_X), 1 - lax.rem(i, N_CORE)
        return lax.rem(x + sign * dx + N_X, N_X) * N_CORE + lax.rem(core + dc, N_CORE)

    def loop(lo, hi, body):
        def step(i, carry):
            body(i)
            return carry

        lax.fori_loop(lo, hi, step, 0)

    def group_copy(i, landing, ss, rs):
        return pltpu.make_async_remote_copy(
            src_ref=send_v.at[i], dst_ref=landing.at[i], send_sem=ss.at[i], recv_sem=rs.at[i],
            device_id={"grp": group_at(i, 1)}, device_id_type=MESH,
        )

    def loop_copy(i, landing, ss, rs):
        return pltpu.make_async_remote_copy(
            src_ref=send_v.at[N_GRP + i], dst_ref=landing.at[N_GRP + i],
            send_sem=ss.at[N_GRP + i], recv_sem=rs.at[N_GRP + i],
            device_id={"blk": loop_at(i, 1)}, device_id_type=MESH,
        )

    fetch_hist = pltpu.make_async_copy(hist_h, hist_v, in_sem.at[0])
    fetch_val = pltpu.make_async_copy(val_h, val_v.at[pl.ds(0, NONE)], in_sem.at[1])
    fetch_feat = pltpu.make_async_copy(feat_h, feat_v, in_sem.at[2])
    fetch_init = pltpu.make_async_copy(init_h, init_v, in_sem.at[3])
    fetch_hist.start()
    barrier = pltpu.get_barrier_semaphore()

    def greet_group(i):
        pl.semaphore_signal(barrier, inc=1, device_id={"grp": group_at(i, 1)}, device_id_type=MESH)

    def greet_loop(i):
        pl.semaphore_signal(barrier, inc=1, device_id={"blk": loop_at(i, 1)}, device_id_type=MESH)

    loop(0, N_GRP - 1, greet_group)
    loop(0, N_BLK - 1, greet_loop)
    fetch_val.start()
    fetch_feat.start()
    fetch_init.start()

    ids = ids_ref[...]
    wide = (TILES, 128)
    tile = lax.broadcasted_iota(jnp.int32, wide, 0)
    slot = lax.broadcasted_iota(jnp.int32, wide, 1)
    entry = lax.broadcasted_iota(jnp.int32, ids.shape, 1)
    last = jnp.full(wide, NONE, jnp.int32)
    prev = jnp.full(ids.shape, ENTRIES, jnp.int32)
    for k in range(ENTRIES):
        column = ids[:, k : k + 1]
        last = jnp.where(column == slot, tile * ENTRIES + k, last)
        prev = jnp.where(jnp.logical_and(column == ids, entry > k), k, prev)
    last_v[...] = jnp.zeros_like(last_v)
    prev_v[...] = jnp.zeros_like(prev_v)
    last_v[pl.ds(0, TILES), :] = last
    prev_v[pl.ds(0, TILES), pl.ds(0, ENTRIES)] = prev
    put_last = pltpu.make_async_copy(last_v, last_s, tab_sem.at[0])
    put_prev = pltpu.make_async_copy(prev_v, prev_s, tab_sem.at[1])
    put_last.start()
    put_prev.start()

    fetch_hist.wait()

    def stage_group(i):
        send_v[i] = hist_v[gt_ref[g, group_at(i, 1)]]

    def stage_loop(i):
        send_v[N_GRP + i] = hist_v[lt_ref[b, loop_at(i, 1)]]

    loop(0, N_GRP - 1, stage_group)
    loop(0, N_BLK - 1, stage_loop)
    pull_v[N_GRP - 1] = hist_v[gt_ref[g, g]]
    pull_v[N_FAR - 1] = hist_v[lt_ref[b, b]]
    put_last.wait()
    put_prev.wait()

    pl.semaphore_wait(barrier, N_GRP + N_BLK - 2)
    loop(0, N_GRP - 1, lambda i: group_copy(i, pull_v, send_sem, recv_sem).start())
    loop(0, N_BLK - 1, lambda i: loop_copy(i, pull_v, send_sem, recv_sem).start())

    fetch_val.wait()
    val_v[NONE] = jnp.zeros((EDGE, EDGE), bf16)
    turned_v[NONE] = jnp.zeros((EDGE, EDGE), bf16)
    chain_v[ENTRIES] = jnp.zeros((EDGE, EDGE), f32)

    def chain_tile(t):
        def chain_entry(k):
            e = t * ENTRIES + k
            total = val_v[e].astype(f32) + chain_v[prev_s[t, k]]
            chain_v[k] = total
            val_v[e] = total.astype(bf16)
            turned_v[e] = jnp.transpose(total).astype(bf16)

        loop(0, ENTRIES, chain_entry)

    loop(0, TILES, chain_tile)

    def lay_out(chunk, slot_of):
        def lay_tile(t):
            rows = pl.ds(pl.multiple_of(t * EDGE, EDGE), EDGE)
            for q in range(CHUNK):
                adj_v[chunk, rows, pl.ds(q * EDGE, EDGE)] = val_v[last_s[t, slot_of(q)]]

        loop(0, TILES, lay_tile)

    def group_slot(i, sign):
        return TILES + group_at(i, sign)

    def loop_slot(i, sign):
        return TILES + N_GRP + loop_at(i, sign)

    loop(0, OWN_CHUNKS, lambda m: lay_out(m, lambda q: m * CHUNK + q))
    loop(0, LOOP_CHUNKS, lambda m: lay_out(OWN_CHUNKS + m, lambda q: loop_slot(m * CHUNK + q, -1)))
    loop(0, GROUP_CHUNKS, lambda m: lay_out(OWN_CHUNKS + LOOP_CHUNKS + m, lambda q: group_slot(m * CHUNK + q, -1)))

    fetch_feat.wait()
    fetch_init.wait()

    def own_block(t):
        own_v[t] = feat_v[t].astype(bf16)
        gath_v[t] = jnp.zeros((EDGE, HIDDEN), f32)

    loop(0, TILES, own_block)

    def gather(chunk, blocks_ref, first):
        right = blocks_ref[pl.ds(first, CHUNK)].reshape(CHUNK * EDGE, HIDDEN)

        def gather_rows(m):
            rows = pl.ds(pl.multiple_of(m * CHUNK * EDGE, CHUNK * EDGE), CHUNK * EDGE)
            part = jnp.dot(adj_v[chunk, rows, :], right, preferred_element_type=f32)
            gath_v[pl.ds(m * CHUNK, CHUNK)] += part.reshape(CHUNK, EDGE, HIDDEN)

        loop(0, TILES // CHUNK, gather_rows)

    loop(0, OWN_CHUNKS, lambda m: gather(m, own_v, m * CHUNK))
    loop(0, N_BLK - 1, lambda i: loop_copy(i, pull_v, send_sem, recv_sem).wait_recv())
    loop(0, LOOP_CHUNKS, lambda m: gather(OWN_CHUNKS + m, pull_v, N_GRP + m * CHUNK))

    def gather_group(m):
        loop(m * CHUNK, m * CHUNK + CHUNK, lambda i: group_copy(i, pull_v, send_sem, recv_sem).wait_recv())
        gather(OWN_CHUNKS + LOOP_CHUNKS + m, pull_v, m * CHUNK)

    loop(0, GROUP_CHUNKS - 1, gather_group)
    final = (GROUP_CHUNKS - 1) * CHUNK
    loop(final, N_GRP - 1, lambda i: group_copy(i, pull_v, send_sem, recv_sem).wait_recv())
    gather(OWN_CHUNKS + LOOP_CHUNKS + GROUP_CHUNKS - 1, pull_v, final)

    def layer(m):
        start = init_v[pl.ds(m * CHUNK, CHUNK)].astype(f32)
        mixed = ((1.0 - teleport) * gath_v[pl.ds(m * CHUNK, CHUNK)] + teleport * start).astype(bf16)
        mixed = mixed.reshape(CHUNK * EDGE, HIDDEN)
        product = jnp.dot(mixed, w_ref[...], preferred_element_type=f32)
        fresh = jnp.maximum((1.0 - mapping_share) * mixed.astype(f32) + mapping_share * product, 0.0)
        out_v[pl.ds(m * CHUNK, CHUNK)] = fresh.reshape(CHUNK, EDGE, HIDDEN)
        left_v[pl.ds(pl.multiple_of(m * CHUNK * EDGE, CHUNK * EDGE), CHUNK * EDGE), :] = fresh.astype(bf16)

    loop(0, TILES // CHUNK, layer)
    loop(0, N_GRP - 1, lambda i: group_copy(i, pull_v, send_sem, recv_sem).wait_send())
    loop(0, N_BLK - 1, lambda i: loop_copy(i, pull_v, send_sem, recv_sem).wait_send())

    def message(c):
        left = jnp.concatenate([turned_v[last_s[t, c]] for t in range(TILES)], axis=1)
        return jnp.dot(left, left_v[...], preferred_element_type=f32).astype(bf16)

    def send_group(i):
        send_v[i] = message(group_slot(i, 1))
        group_copy(i, push_v, send2_sem, recv2_sem).start()

    def send_loop(i):
        send_v[N_GRP + i] = message(loop_slot(i, 1))
        loop_copy(i, push_v, send2_sem, recv2_sem).start()

    loop(0, N_GRP - 1, send_group)
    loop(0, N_BLK - 1, send_loop)
    push_v[N_GRP - 1] = message(TILES + g)
    push_v[N_FAR - 1] = message(TILES + N_GRP + b)
    store_out = pltpu.make_async_copy(out_v, refreshed_h, res_sem.at[0])
    store_out.start()

    def clear(t):
        box_v[t] = jnp.zeros((EDGE, HIDDEN), f32)

    loop(0, TILES, clear)

    def deliver(first, owner_block):
        def deliver_block(t):
            total = box_v[t]
            for q in range(CHUNK):
                total = total + jnp.where(owner_block(q) == t, push_v[first + q].astype(f32), 0.0)
            box_v[t] = total

        loop(0, TILES, deliver_block)

    loop(0, N_BLK - 1, lambda i: loop_copy(i, push_v, send2_sem, recv2_sem).wait_recv())
    loop(0, LOOP_CHUNKS, lambda m: deliver(N_GRP + m * CHUNK, lambda q: lt_ref[b, loop_at(m * CHUNK + q, -1)]))

    def deliver_group(m):
        loop(m * CHUNK, m * CHUNK + CHUNK, lambda i: group_copy(i, push_v, send2_sem, recv2_sem).wait_recv())
        deliver(m * CHUNK, lambda q: gt_ref[g, group_at(m * CHUNK + q, -1)])

    loop(0, GROUP_CHUNKS - 1, deliver_group)
    loop(final, N_GRP - 1, lambda i: group_copy(i, push_v, send2_sem, recv2_sem).wait_recv())
    deliver(final, lambda q: gt_ref[g, group_at(final + q, -1)])
    store_box = pltpu.make_async_copy(box_v, inbox_h, res_sem.at[1])
    store_box.start()
    loop(0, N_GRP - 1, lambda i: group_copy(i, push_v, send2_sem, recv2_sem).wait_send())
    loop(0, N_BLK - 1, lambda i: loop_copy(i, push_v, send2_sem, recv2_sem).wait_send())
    store_out.wait()
    store_box.wait()


def body(features, initial, history, weight, column_ids, block_values, group_table, loop_table):
    f32, bf16, i32 = jnp.float32, jnp.bfloat16, jnp.int32
    blocks = (TILES, EDGE, HIDDEN)
    any_space = pl.BlockSpec(memory_space=pl.ANY)
    vmem, smem = pl.BlockSpec(memory_space=pltpu.VMEM), pl.BlockSpec(memory_space=pltpu.SMEM)
    dma = pltpu.SemaphoreType.DMA
    refreshed, inbox = pl.pallas_call(
        kernel,
        out_shape=[jax.ShapeDtypeStruct(blocks, f32)] * 2,
        in_specs=[any_space, any_space, any_space, vmem, vmem, any_space, smem, smem],
        out_specs=[any_space, any_space],
        scratch_shapes=[
            pltpu.VMEM(blocks, bf16),
            pltpu.VMEM(blocks, f32),
            pltpu.VMEM(blocks, bf16),
            pltpu.VMEM(blocks, bf16),
            pltpu.VMEM((NONE + 1, EDGE, EDGE), bf16),
            pltpu.VMEM((ENTRIES + 1, EDGE, EDGE), f32),
            pltpu.VMEM((NONE + 1, EDGE, EDGE), bf16),
            pltpu.VMEM((OWN_CHUNKS + LOOP_CHUNKS + GROUP_CHUNKS, ROWS, CHUNK * EDGE), bf16),
            pltpu.VMEM((N_FAR, EDGE, HIDDEN), bf16),
            pltpu.VMEM((N_FAR, EDGE, HIDDEN), bf16),
            pltpu.VMEM((N_FAR, EDGE, HIDDEN), bf16),
            pltpu.VMEM(blocks, f32),
            pltpu.VMEM(blocks, f32),
            pltpu.VMEM((ROWS, HIDDEN), bf16),
            pltpu.VMEM(blocks, f32),
            pltpu.VMEM((16, 128), i32),
            pltpu.VMEM((16, 128), i32),
            pltpu.SMEM((16, 128), i32),
            pltpu.SMEM((16, 128), i32),
            dma((4,)),
            dma((2,)),
            dma((N_FAR,)),
            dma((N_FAR,)),
            dma((N_FAR,)),
            dma((N_FAR,)),
            dma((2,)),
        ],
        compiler_params=pltpu.CompilerParams(
            collective_id=0, has_side_effects=True, vmem_limit_bytes=64 * 2**20 - 2**16
        ),
    )(
        features.reshape(blocks),
        initial.reshape(blocks),
        history.reshape(blocks),
        weight,
        column_ids,
        block_values.reshape(NONE, EDGE, EDGE),
        group_table[0],
        loop_table[0],
    )
    return refreshed.reshape(ROWS, HIDDEN), inbox.reshape(ROWS, HIDDEN)


def solution(mesh):
    in_specs = (
        P(("blk", "grp"), None),
        P(("blk", "grp"), None),
        P(("blk", "grp"), None),
        P(),
        P(("blk", "grp"), None),
        P(("blk", "grp"), None, None, None),
        P("blk", None, None),
        P("grp", None, None),
    )
    out_specs = (P(("blk", "grp"), None), P(("blk", "grp"), None))
    return jax.shard_map(body, mesh=mesh, in_specs=in_specs, out_specs=out_specs, check_vma=False)
```

```python
import jax
import jax.numpy as jnp
from jax import lax
from jax.experimental import pallas as pl
from jax.experimental.pallas import tpu as pltpu
from jax.sharding import PartitionSpec as P

MESH = pl.DeviceIdType.MESH
teleport = 0.1
mapping_share = 0.5

TILES, ENTRIES, EDGE, HIDDEN = 12, 16, 128, 256
N_Z, N_Y, N_X, N_CORE = 8, 4, 4, 2
N_GRP, N_BLK = N_Z * N_Y, N_X * N_CORE
N_FAR = N_GRP + N_BLK
SELF = N_Z - 1
Y_LINE = N_GRP - (N_Y - 1)
PAIR = 2
OWN_PAIRS, LOOP_PAIRS, GROUP_PAIRS = TILES // PAIR, N_BLK // PAIR, N_GRP // PAIR
BAND = 6
ROWS = TILES * EDGE
NONE = TILES * ENTRIES


def far_first(k, n):
    return lax.rem(n // 2 + (1 - 2 * lax.rem(k, 2)) * lax.div(k + 1, 2) + n, n)


def kernel(
    feat_h, init_h, hist_h, w_h, ids_h, val_h, gt_h, lt_h,
    out_v, box_v,
    hist_v, init_v, w_v, ids_v, own_v, val_v, low_v, chain_v, adj_v, send_v, pull_v, push_v,
    left_v, last_v, prev_v, last_s, prev_s, gt_s, lt_s,
    in_sem, tab_sem, line_sem, send_sem, recv_sem, send2_sem, recv2_sem,
):
    f32, bf16 = jnp.float32, jnp.bfloat16
    g, b = lax.axis_index("grp"), lax.axis_index("blk")
    z, y = lax.div(g, N_Y), lax.rem(g, N_Y)
    x, core = lax.div(b, N_CORE), lax.rem(b, N_CORE)
    gath_v = box_v

    def group_of(dz, dy, sign):
        return lax.rem(z + sign * dz + N_Z, N_Z) * N_Y + lax.rem(y + sign * dy + N_Y, N_Y)

    def group_at(i, sign):
        r = jnp.maximum(i - N_Z, 0)
        on_z, on_y = i < N_Z, i >= Y_LINE
        dz = jnp.where(on_z, far_first(i, N_Z), jnp.where(on_y, 0, far_first(lax.div(r, N_Y - 1), N_Z)))
        dy = jnp.where(on_z, 0, far_first(lax.rem(r, N_Y - 1), N_Y))
        return group_of(dz, dy, sign)

    def loop_at(i, sign):
        dx, dc = far_first(lax.div(i, N_CORE), N_X), 1 - lax.rem(i, N_CORE)
        return lax.rem(x + sign * dx + N_X, N_X) * N_CORE + lax.rem(core + dc, N_CORE)

    def loop(lo, hi, body, unroll=1):
        def step(i, carry):
            for u in range(unroll):
                body(lo + i * unroll + u)
            return carry

        lax.fori_loop(0, (hi - lo) // unroll, step, 0)

    def group_copy(i, landing, ss, rs):
        return pltpu.make_async_remote_copy(
            src_ref=send_v.at[i], dst_ref=landing.at[i], send_sem=ss.at[i], recv_sem=rs.at[i],
            device_id={"grp": group_at(i, 1)}, device_id_type=MESH,
        )

    def loop_copy(i, landing, ss, rs):
        return pltpu.make_async_remote_copy(
            src_ref=send_v.at[N_GRP + i], dst_ref=landing.at[N_GRP + i],
            send_sem=ss.at[N_GRP + i], recv_sem=rs.at[N_GRP + i],
            device_id={"blk": loop_at(i, 1)}, device_id_type=MESH,
        )

    fetch_hist = pltpu.make_async_copy(hist_h, hist_v, in_sem.at[0])
    fetch_gt = pltpu.make_async_copy(gt_h, gt_s, in_sem.at[1])
    fetch_lt = pltpu.make_async_copy(lt_h, lt_s, in_sem.at[2])
    fetch_ids = pltpu.make_async_copy(ids_h, ids_v, in_sem.at[3])
    fetch_val = pltpu.make_async_copy(val_h, val_v.at[pl.ds(0, NONE)], in_sem.at[4])
    fetch_feat = pltpu.make_async_copy(feat_h, out_v, in_sem.at[5])
    fetch_init = pltpu.make_async_copy(init_h, init_v, in_sem.at[6])
    fetch_w = pltpu.make_async_copy(w_h, w_v, in_sem.at[7])
    for fetch in (fetch_gt, fetch_lt, fetch_hist, fetch_ids):
        fetch.start()
    barrier = pltpu.get_barrier_semaphore()

    def greet_group(i):
        pl.semaphore_signal(barrier, inc=1, device_id={"grp": group_at(i, 1)}, device_id_type=MESH)

    def greet_loop(i):
        pl.semaphore_signal(barrier, inc=1, device_id={"blk": loop_at(i, 1)}, device_id_type=MESH)

    loop(0, SELF, greet_group)
    loop(Y_LINE, N_GRP, greet_group)
    loop(0, N_BLK - 1, greet_loop)
    for fetch in (fetch_val, fetch_feat, fetch_init, fetch_w):
        fetch.start()

    fetch_gt.wait()
    fetch_lt.wait()
    fetch_hist.wait()

    def stage_group(i):
        send_v[i] = hist_v[gt_s[g, group_at(i, 1)]]

    def stage_loop(i):
        send_v[N_GRP + i] = hist_v[lt_s[b, loop_at(i, 1)]]

    loop(0, SELF, stage_group)
    loop(SELF + 1, N_GRP, stage_group)
    loop(0, N_BLK - 1, stage_loop)
    pull_v[SELF] = hist_v[gt_s[g, g]]
    pull_v[N_FAR - 1] = hist_v[lt_s[b, b]]

    def pull_group(i):
        group_copy(i, pull_v, send_sem, recv_sem).start()

    pl.semaphore_wait(barrier, (N_Z - 1) + (N_Y - 1) + (N_BLK - 1))

    def greet_line(i):
        pl.semaphore_signal(line_sem, inc=1, device_id={"grp": group_at(i, 1)}, device_id_type=MESH)

    loop(Y_LINE, N_GRP, greet_line)
    loop(0, SELF, pull_group)
    loop(Y_LINE, N_GRP, pull_group)
    loop(0, N_BLK - 1, lambda i: loop_copy(i, pull_v, send_sem, recv_sem).start())
    pl.semaphore_wait(line_sem, N_Y - 1)
    loop(N_Z, Y_LINE, pull_group)

    fetch_ids.wait()
    ids = ids_v[...]
    wide = (TILES, 128)
    tile = lax.broadcasted_iota(jnp.int32, wide, 0)
    slot = lax.broadcasted_iota(jnp.int32, wide, 1)
    entry = lax.broadcasted_iota(jnp.int32, ids.shape, 1)
    last = jnp.full(wide, NONE, jnp.int32)
    prev = jnp.full(ids.shape, ENTRIES, jnp.int32)
    for k in range(ENTRIES):
        column = ids[:, k : k + 1]
        last = jnp.where(column == slot, tile * ENTRIES + k, last)
        prev = jnp.where(jnp.logical_and(column == ids, entry > k), k, prev)
    last_v[...] = jnp.zeros_like(last_v)
    prev_v[...] = jnp.zeros_like(prev_v)
    last_v[pl.ds(0, TILES), :] = last
    prev_v[pl.ds(0, TILES), pl.ds(0, ENTRIES)] = prev
    put_last = pltpu.make_async_copy(last_v, last_s, tab_sem.at[0])
    put_prev = pltpu.make_async_copy(prev_v, prev_s, tab_sem.at[1])
    put_last.start()
    put_prev.start()
    put_last.wait()
    put_prev.wait()

    fetch_val.wait()
    for none in (val_v, low_v):
        none[NONE] = jnp.zeros((EDGE, EDGE), bf16)
    chain_v[ENTRIES] = jnp.zeros((EDGE, EDGE), f32)

    def chain_tile(t):
        def chain_entry(k):
            e = t * ENTRIES + k
            total = val_v[e].astype(f32) + chain_v[prev_s[t, k]]
            high = total.astype(bf16)
            chain_v[k] = total
            val_v[e] = high
            low_v[e] = (total - high.astype(f32)).astype(bf16)

        loop(0, ENTRIES, chain_entry, 4)

    loop(0, TILES, chain_tile)

    def group_slot(i, sign):
        return TILES + group_at(i, sign)

    def loop_slot(i, sign):
        return TILES + N_GRP + loop_at(i, sign)

    def lay_out(pair, first, second):
        def lay_tile(t):
            rows = pl.ds(pl.multiple_of(t * EDGE, EDGE), EDGE)
            for q, c in enumerate((first, second)):
                e = last_s[t, c]
                adj_v[pair, rows, pl.ds(q * EDGE, EDGE)] = val_v[e]
                adj_v[pair, rows, pl.ds((PAIR + q) * EDGE, EDGE)] = low_v[e]

        loop(0, TILES, lay_tile, 4)

    fetch_feat.wait()

    def own_block(t):
        own_v[t] = out_v[t].astype(bf16)
        gath_v[t] = jnp.zeros((EDGE, HIDDEN), f32)

    loop(0, TILES, own_block)

    def product_of(pair, blocks_ref, first, m):
        right = blocks_ref[pl.ds(first, PAIR)].reshape(PAIR * EDGE, HIDDEN)
        right = jnp.concatenate([right, right], axis=0)
        rows = pl.ds(pl.multiple_of(m * BAND * EDGE, BAND * EDGE), BAND * EDGE)
        part = jnp.dot(adj_v[pair, rows, :], right, preferred_element_type=f32)
        return part.reshape(BAND, EDGE, HIDDEN)

    def gather(pair, blocks_ref, first, pairs=1):
        def gather_rows(m):
            part = product_of(pair, blocks_ref, first, m)
            for extra in range(1, pairs):
                part = part + product_of(pair + extra, blocks_ref, first + extra * PAIR, m)
            gath_v[pl.ds(m * BAND, BAND)] += part

        loop(0, TILES // BAND, gather_rows)

    loop(0, OWN_PAIRS, lambda p: lay_out(p, p * PAIR, p * PAIR + 1))
    loop(0, OWN_PAIRS // 2, lambda p: gather(2 * p, own_v, 2 * p * PAIR, 2))
    loop(0, N_BLK - 1, lambda i: loop_copy(i, pull_v, send_sem, recv_sem).wait_recv())

    loop(0, LOOP_PAIRS, lambda p: lay_out(p, loop_slot(p * PAIR, -1), loop_slot(p * PAIR + 1, -1)))
    loop(0, LOOP_PAIRS // 2, lambda p: gather(2 * p, pull_v, N_GRP + 2 * p * PAIR, 2))
    loop(0, GROUP_PAIRS, lambda p: lay_out(p, group_slot(p * PAIR, -1), group_slot(p * PAIR + 1, -1)))
    fetch_init.wait()
    fetch_w.wait()

    def pulled_group(i):
        group_copy(i, pull_v, send_sem, recv_sem).wait_recv()

    def gather_group(p):
        loop(2 * p * PAIR, 2 * p * PAIR + 2 * PAIR, pulled_group)
        gather(2 * p, pull_v, 2 * p * PAIR, 2)

    loop(Y_LINE, N_GRP, pulled_group)
    gather(GROUP_PAIRS - 1, pull_v, N_GRP - PAIR)
    gather_group(0)
    loop(SELF - 3, SELF, pulled_group)
    gather(SELF // PAIR - 1, pull_v, SELF - 3, 2)
    loop(2, GROUP_PAIRS // 2 - 1, gather_group)
    pulled_group(Y_LINE - 1)

    def layer(m):
        gathered = gath_v[pl.ds(m * BAND, BAND)] + product_of(GROUP_PAIRS - 2, pull_v, Y_LINE - 1, m)
        start = init_v[pl.ds(m * BAND, BAND)].astype(f32)
        mixed = ((1.0 - teleport) * gathered + teleport * start).astype(bf16)
        mixed = mixed.reshape(BAND * EDGE, HIDDEN)
        product = jnp.dot(mixed, w_v[...], preferred_element_type=f32)
        fresh = jnp.maximum((1.0 - mapping_share) * mixed.astype(f32) + mapping_share * product, 0.0)
        out_v[pl.ds(m * BAND, BAND)] = fresh.reshape(BAND, EDGE, HIDDEN)
        left_v[pl.ds(pl.multiple_of(m * BAND * EDGE, BAND * EDGE), BAND * EDGE), :] = fresh.astype(bf16)

    loop(0, TILES // BAND, layer)

    def message(c):
        left = jnp.concatenate([val_v[last_s[t, c]] for t in range(TILES)], axis=0)
        total = lax.dot_general(left, left_v[...], (((0,), (0,)), ((), ())), preferred_element_type=f32)
        return total.astype(bf16)

    def send_group(i):
        group_copy(i, pull_v, send_sem, recv_sem).wait_send()
        send_v[i] = message(group_slot(i, 1))
        group_copy(i, push_v, send2_sem, recv2_sem).start()

    def send_loop(i):
        loop_copy(i, pull_v, send_sem, recv_sem).wait_send()
        send_v[N_GRP + i] = message(loop_slot(i, 1))
        loop_copy(i, push_v, send2_sem, recv2_sem).start()

    loop(0, SELF, send_group)
    loop(N_Z, N_GRP, send_group)
    loop(0, N_BLK - 1, send_loop)
    push_v[SELF] = message(TILES + g)
    push_v[N_FAR - 1] = message(TILES + N_GRP + b)

    def clear(t):
        box_v[t] = jnp.zeros((EDGE, HIDDEN), f32)

    loop(0, TILES, clear)

    def deliver(first, owner_block):
        owners = [owner_block(q) for q in range(PAIR)]

        def deliver_rows(r):
            rows = pl.ds(pl.multiple_of(r * 16, 16), 16)
            parts = [push_v[first + q, rows, :].astype(f32) for q in range(PAIR)]
            for t in range(TILES):
                total = box_v[t, rows, :]
                for q in range(PAIR):
                    total = total + jnp.where(owners[q] == t, parts[q], 0.0)
                box_v[t, rows, :] = total

        loop(0, EDGE // 16, deliver_rows)

    def pushed_group(i):
        group_copy(i, push_v, send2_sem, recv2_sem).wait_recv()

    def deliver_pair(p):
        deliver(p * PAIR, lambda q: gt_s[g, group_at(p * PAIR + q, -1)])

    def deliver_group(p):
        loop(p * PAIR, p * PAIR + PAIR, pushed_group)
        deliver_pair(p)

    loop(0, N_BLK - 1, lambda i: loop_copy(i, push_v, send2_sem, recv2_sem).wait_recv())
    loop(0, LOOP_PAIRS, lambda p: deliver(N_GRP + p * PAIR, lambda q: lt_s[b, loop_at(p * PAIR + q, -1)]))
    loop(Y_LINE, N_GRP, pushed_group)
    deliver_pair(GROUP_PAIRS - 1)
    loop(0, SELF // PAIR, deliver_group)
    pushed_group(SELF - 1)
    deliver_pair(SELF // PAIR)
    loop(N_Z // PAIR, GROUP_PAIRS - 2, deliver_group)
    pushed_group(Y_LINE - 1)
    deliver_pair(GROUP_PAIRS - 2)

    def sent_group(i):
        group_copy(i, push_v, send2_sem, recv2_sem).wait_send()

    loop(0, SELF, sent_group)
    loop(N_Z, N_GRP, sent_group)
    loop(0, N_BLK - 1, lambda i: loop_copy(i, push_v, send2_sem, recv2_sem).wait_send())


def body(features, initial, history, weight, column_ids, block_values, group_table, loop_table):
    f32, bf16, i32 = jnp.float32, jnp.bfloat16, jnp.int32
    blocks = (TILES, EDGE, HIDDEN)
    any_space, vmem = pl.BlockSpec(memory_space=pl.ANY), pl.BlockSpec(memory_space=pltpu.VMEM)
    dma = pltpu.SemaphoreType.DMA
    far = (N_FAR, EDGE, HIDDEN)
    refreshed, inbox = pl.pallas_call(
        kernel,
        out_shape=[pltpu.VMEM(blocks, f32)] * 2,
        in_specs=[any_space] * 8,
        out_specs=[vmem, vmem],
        scratch_shapes=[
            pltpu.VMEM(blocks, bf16),
            pltpu.VMEM(blocks, bf16),
            pltpu.VMEM((HIDDEN, HIDDEN), bf16),
            pltpu.VMEM((TILES, ENTRIES), i32),
            pltpu.VMEM(blocks, bf16),
            pltpu.VMEM((NONE + 1, EDGE, EDGE), bf16),
            pltpu.VMEM((NONE + 1, EDGE, EDGE), bf16),
            pltpu.VMEM((ENTRIES + 1, EDGE, EDGE), f32),
            pltpu.VMEM((GROUP_PAIRS, ROWS, 2 * PAIR * EDGE), bf16),
            pltpu.VMEM(far, bf16),
            pltpu.VMEM(far, bf16),
            pltpu.VMEM(far, bf16),
            pltpu.VMEM((ROWS, HIDDEN), bf16),
            pltpu.VMEM((16, 128), i32),
            pltpu.VMEM((16, 128), i32),
            pltpu.SMEM((16, 128), i32),
            pltpu.SMEM((16, 128), i32),
            pltpu.SMEM((N_GRP, N_GRP), i32),
            pltpu.SMEM((N_BLK, N_BLK), i32),
            dma((8,)),
            dma((2,)),
            pltpu.SemaphoreType.REGULAR,
            dma((N_FAR,)),
            dma((N_FAR,)),
            dma((N_FAR,)),
            dma((N_FAR,)),
        ],
        compiler_params=pltpu.CompilerParams(
            collective_id=0, has_side_effects=True, vmem_limit_bytes=60 * 2**20
        ),
    )(
        features.reshape(blocks),
        initial.reshape(blocks),
        history.reshape(blocks),
        weight,
        column_ids,
        block_values.reshape(NONE, EDGE, EDGE),
        group_table[0],
        loop_table[0],
    )
    return refreshed.reshape(ROWS, HIDDEN), inbox.reshape(ROWS, HIDDEN)


def solution(mesh):
    in_specs = (
        P(("blk", "grp"), None),
        P(("blk", "grp"), None),
        P(("blk", "grp"), None),
        P(),
        P(("blk", "grp"), None),
        P(("blk", "grp"), None, None, None),
        P("blk", None, None),
        P("grp", None, None),
    )
    out_specs = (P(("blk", "grp"), None), P(("blk", "grp"), None))
    return jax.shard_map(body, mesh=mesh, in_specs=in_specs, out_specs=out_specs, check_vma=False)
```

```python
import jax
import jax.numpy as jnp
from jax import lax
from jax.experimental import pallas as pl
from jax.experimental.pallas import tpu as pltpu
from jax.sharding import PartitionSpec as P

MESH = pl.DeviceIdType.MESH
teleport = 0.1
mapping_share = 0.5

TILES, ENTRIES, EDGE, HIDDEN = 12, 16, 128, 256
N_Z, N_Y, N_X, N_CORE = 8, 4, 4, 2
N_GRP, N_BLK = N_Z * N_Y, N_X * N_CORE
N_FAR = N_GRP + N_BLK
SELF = N_Z - 1
Y_LINE = N_GRP - (N_Y - 1)
PAIR = 2
OWN_PAIRS, LOOP_PAIRS, GROUP_PAIRS = TILES // PAIR, N_BLK // PAIR, N_GRP // PAIR
BAND = 6
ROWS = TILES * EDGE
NONE = TILES * ENTRIES


def far_first(k, n):
    return lax.rem(n // 2 + (1 - 2 * lax.rem(k, 2)) * lax.div(k + 1, 2) + n, n)


def kernel(
    feat_h, init_h, hist_h, w_h, ids_h, val_h, gt_h, lt_h,
    out_v, box_v,
    hist_v, init_v, w_v, ids_v, own_v, val_v, low_v, chain_v, adj_v, send_v, pull_v, push_v,
    left_v, last_v, prev_v, last_s, prev_s, gt_s, lt_s,
    in_sem, tab_sem, line_sem, send_sem, recv_sem, send2_sem, recv2_sem,
):
    f32, bf16 = jnp.float32, jnp.bfloat16
    g, b = lax.axis_index("grp"), lax.axis_index("blk")
    z, y = lax.div(g, N_Y), lax.rem(g, N_Y)
    x, core = lax.div(b, N_CORE), lax.rem(b, N_CORE)
    gath_v = box_v

    def group_of(dz, dy, sign):
        return lax.rem(z + sign * dz + N_Z, N_Z) * N_Y + lax.rem(y + sign * dy + N_Y, N_Y)

    def group_at(i, sign):
        r = jnp.maximum(i - N_Z, 0)
        on_z, on_y = i < N_Z, i >= Y_LINE
        dz = jnp.where(on_z, far_first(i, N_Z), jnp.where(on_y, 0, far_first(lax.div(r, N_Y - 1), N_Z)))
        dy = jnp.where(on_z, 0, far_first(lax.rem(r, N_Y - 1), N_Y))
        return group_of(dz, dy, sign)

    def loop_at(i, sign):
        dx, dc = far_first(lax.div(i, N_CORE), N_X), 1 - lax.rem(i, N_CORE)
        return lax.rem(x + sign * dx + N_X, N_X) * N_CORE + lax.rem(core + dc, N_CORE)

    def loop(lo, hi, body, unroll=1):
        def step(i, carry):
            for u in range(unroll):
                body(lo + i * unroll + u)
            return carry

        lax.fori_loop(0, (hi - lo) // unroll, step, 0)

    def group_copy(i, landing, ss, rs):
        return pltpu.make_async_remote_copy(
            src_ref=send_v.at[i], dst_ref=landing.at[i], send_sem=ss.at[i], recv_sem=rs.at[i],
            device_id={"grp": group_at(i, 1)}, device_id_type=MESH,
        )

    def loop_copy(i, landing, ss, rs):
        return pltpu.make_async_remote_copy(
            src_ref=send_v.at[N_GRP + i], dst_ref=landing.at[N_GRP + i],
            send_sem=ss.at[N_GRP + i], recv_sem=rs.at[N_GRP + i],
            device_id={"blk": loop_at(i, 1)}, device_id_type=MESH,
        )

    fetch_hist = pltpu.make_async_copy(hist_h, hist_v, in_sem.at[0])
    fetch_gt = pltpu.make_async_copy(gt_h, gt_s, in_sem.at[1])
    fetch_lt = pltpu.make_async_copy(lt_h, lt_s, in_sem.at[2])
    fetch_ids = pltpu.make_async_copy(ids_h, ids_v, in_sem.at[3])
    fetch_val = pltpu.make_async_copy(val_h, val_v.at[pl.ds(0, NONE)], in_sem.at[4])
    fetch_feat = pltpu.make_async_copy(feat_h, out_v, in_sem.at[5])
    fetch_init = pltpu.make_async_copy(init_h, init_v, in_sem.at[6])
    fetch_w = pltpu.make_async_copy(w_h, w_v, in_sem.at[7])
    for fetch in (fetch_gt, fetch_lt, fetch_hist, fetch_ids):
        fetch.start()
    barrier = pltpu.get_barrier_semaphore()

    def greet_group(i):
        pl.semaphore_signal(barrier, inc=1, device_id={"grp": group_at(i, 1)}, device_id_type=MESH)

    def greet_loop(i):
        pl.semaphore_signal(barrier, inc=1, device_id={"blk": loop_at(i, 1)}, device_id_type=MESH)

    loop(0, SELF, greet_group)
    loop(Y_LINE, N_GRP, greet_group)
    loop(0, N_BLK - 1, greet_loop)
    for fetch in (fetch_val, fetch_feat, fetch_init, fetch_w):
        fetch.start()

    fetch_gt.wait()
    fetch_lt.wait()
    fetch_hist.wait()

    def stage_group(i):
        send_v[i] = hist_v[gt_s[g, group_at(i, 1)]]

    def stage_loop(i):
        send_v[N_GRP + i] = hist_v[lt_s[b, loop_at(i, 1)]]

    loop(0, SELF, stage_group)
    loop(SELF + 1, N_GRP, stage_group)
    loop(0, N_BLK - 1, stage_loop)
    pull_v[SELF] = hist_v[gt_s[g, g]]
    pull_v[N_FAR - 1] = hist_v[lt_s[b, b]]

    def pull_group(i):
        group_copy(i, pull_v, send_sem, recv_sem).start()

    pl.semaphore_wait(barrier, (N_Z - 1) + (N_Y - 1) + (N_BLK - 1))

    def greet_line(i):
        pl.semaphore_signal(line_sem, inc=1, device_id={"grp": group_at(i, 1)}, device_id_type=MESH)

    loop(Y_LINE, N_GRP, greet_line)
    loop(0, SELF, pull_group)
    loop(Y_LINE, N_GRP, pull_group)
    loop(0, N_BLK - 1, lambda i: loop_copy(i, pull_v, send_sem, recv_sem).start())
    pl.semaphore_wait(line_sem, N_Y - 1)
    loop(N_Z, Y_LINE, pull_group)

    fetch_ids.wait()
    ids = ids_v[...]
    wide = (TILES, 128)
    tile = lax.broadcasted_iota(jnp.int32, wide, 0)
    slot = lax.broadcasted_iota(jnp.int32, wide, 1)
    entry = lax.broadcasted_iota(jnp.int32, ids.shape, 1)
    last = jnp.full(wide, NONE, jnp.int32)
    prev = jnp.full(ids.shape, ENTRIES, jnp.int32)
    for k in range(ENTRIES):
        column = ids[:, k : k + 1]
        last = jnp.where(column == slot, tile * ENTRIES + k, last)
        prev = jnp.where(jnp.logical_and(column == ids, entry > k), k, prev)
    last_v[...] = jnp.zeros_like(last_v)
    prev_v[...] = jnp.zeros_like(prev_v)
    last_v[pl.ds(0, TILES), :] = last
    prev_v[pl.ds(0, TILES), pl.ds(0, ENTRIES)] = prev
    put_last = pltpu.make_async_copy(last_v, last_s, tab_sem.at[0])
    put_prev = pltpu.make_async_copy(prev_v, prev_s, tab_sem.at[1])
    put_last.start()
    put_prev.start()
    put_last.wait()
    put_prev.wait()

    fetch_val.wait()
    for none in (val_v, low_v):
        none[NONE] = jnp.zeros((EDGE, EDGE), bf16)
    chain_v[ENTRIES] = jnp.zeros((EDGE, EDGE), f32)

    def chain_tile(t):
        def chain_entry(k):
            e = t * ENTRIES + k
            total = val_v[e].astype(f32) + chain_v[prev_s[t, k]]
            high = total.astype(bf16)
            chain_v[k] = total
            val_v[e] = high
            low_v[e] = (total - high.astype(f32)).astype(bf16)

        loop(0, ENTRIES, chain_entry, 4)

    loop(0, TILES, chain_tile)

    def group_slot(i, sign):
        return TILES + group_at(i, sign)

    def loop_slot(i, sign):
        return TILES + N_GRP + loop_at(i, sign)

    def lay_out(pair, first, second):
        def lay_tile(t):
            rows = pl.ds(pl.multiple_of(t * EDGE, EDGE), EDGE)
            for q, c in enumerate((first, second)):
                e = last_s[t, c]
                adj_v[pair, rows, pl.ds(q * EDGE, EDGE)] = val_v[e]
                adj_v[pair, rows, pl.ds((PAIR + q) * EDGE, EDGE)] = low_v[e]

        loop(0, TILES, lay_tile, 4)

    fetch_feat.wait()

    def own_block(t):
        own_v[t] = out_v[t].astype(bf16)
        gath_v[t] = jnp.zeros((EDGE, HIDDEN), f32)

    loop(0, TILES, own_block)

    def product_of(pair, blocks_ref, first, m):
        right = blocks_ref[pl.ds(first, PAIR)].reshape(PAIR * EDGE, HIDDEN)
        right = jnp.concatenate([right, right], axis=0)
        rows = pl.ds(pl.multiple_of(m * BAND * EDGE, BAND * EDGE), BAND * EDGE)
        part = jnp.dot(adj_v[pair, rows, :], right, preferred_element_type=f32)
        return part.reshape(BAND, EDGE, HIDDEN)

    def gather(pair, blocks_ref, first, pairs=1):
        def gather_rows(m):
            part = product_of(pair, blocks_ref, first, m)
            for extra in range(1, pairs):
                part = part + product_of(pair + extra, blocks_ref, first + extra * PAIR, m)
            gath_v[pl.ds(m * BAND, BAND)] += part

        loop(0, TILES // BAND, gather_rows)

    loop(0, OWN_PAIRS, lambda p: lay_out(p, p * PAIR, p * PAIR + 1))
    loop(0, OWN_PAIRS // 2, lambda p: gather(2 * p, own_v, 2 * p * PAIR, 2))
    loop(0, N_BLK - 1, lambda i: loop_copy(i, pull_v, send_sem, recv_sem).wait_recv())

    loop(0, LOOP_PAIRS, lambda p: lay_out(p, loop_slot(p * PAIR, -1), loop_slot(p * PAIR + 1, -1)))
    loop(0, LOOP_PAIRS // 2, lambda p: gather(2 * p, pull_v, N_GRP + 2 * p * PAIR, 2))
    loop(0, GROUP_PAIRS, lambda p: lay_out(p, group_slot(p * PAIR, -1), group_slot(p * PAIR + 1, -1)))
    fetch_init.wait()
    fetch_w.wait()

    def pulled_group(i):
        group_copy(i, pull_v, send_sem, recv_sem).wait_recv()

    def gather_group(p):
        loop(2 * p * PAIR, 2 * p * PAIR + 2 * PAIR, pulled_group)
        gather(2 * p, pull_v, 2 * p * PAIR, 2)

    loop(Y_LINE, N_GRP, pulled_group)
    gather(GROUP_PAIRS - 1, pull_v, N_GRP - PAIR)
    gather_group(0)
    loop(SELF - 3, SELF, pulled_group)
    gather(SELF // PAIR - 1, pull_v, SELF - 3, 2)
    loop(2, GROUP_PAIRS // 2 - 1, gather_group)
    pulled_group(Y_LINE - 1)

    def layer(m):
        gathered = gath_v[pl.ds(m * BAND, BAND)] + product_of(GROUP_PAIRS - 2, pull_v, Y_LINE - 1, m)
        start = init_v[pl.ds(m * BAND, BAND)].astype(f32)
        mixed = ((1.0 - teleport) * gathered + teleport * start).astype(bf16)
        mixed = mixed.reshape(BAND * EDGE, HIDDEN)
        product = jnp.dot(mixed, w_v[...], preferred_element_type=f32)
        fresh = jnp.maximum((1.0 - mapping_share) * mixed.astype(f32) + mapping_share * product, 0.0)
        out_v[pl.ds(m * BAND, BAND)] = fresh.reshape(BAND, EDGE, HIDDEN)
        left_v[pl.ds(pl.multiple_of(m * BAND * EDGE, BAND * EDGE), BAND * EDGE), :] = fresh.astype(bf16)

    loop(0, TILES // BAND, layer, 2)

    def message(c):
        left = jnp.concatenate([val_v[last_s[t, c]] for t in range(TILES)], axis=0)
        total = lax.dot_general(left, left_v[...], (((0,), (0,)), ((), ())), preferred_element_type=f32)
        return total.astype(bf16)

    def send_group(i):
        group_copy(i, pull_v, send_sem, recv_sem).wait_send()
        send_v[i] = message(group_slot(i, 1))
        group_copy(i, push_v, send2_sem, recv2_sem).start()

    def send_loop(i):
        loop_copy(i, pull_v, send_sem, recv_sem).wait_send()
        send_v[N_GRP + i] = message(loop_slot(i, 1))
        loop_copy(i, push_v, send2_sem, recv2_sem).start()

    loop(0, SELF, send_group)
    loop(N_Z, N_GRP, send_group)
    loop(0, N_BLK - 1, send_loop)
    push_v[SELF] = message(TILES + g)
    push_v[N_FAR - 1] = message(TILES + N_GRP + b)

    def clear(t):
        box_v[t] = jnp.zeros((EDGE, HIDDEN), f32)

    loop(0, TILES, clear)

    def deliver(first, owner_block):
        owners = [owner_block(q) for q in range(PAIR)]

        def deliver_rows(r):
            rows = pl.ds(pl.multiple_of(r * 16, 16), 16)
            parts = [push_v[first + q, rows, :].astype(f32) for q in range(PAIR)]
            for t in range(TILES):
                total = box_v[t, rows, :]
                for q in range(PAIR):
                    total = total + jnp.where(owners[q] == t, parts[q], 0.0)
                box_v[t, rows, :] = total

        loop(0, EDGE // 16, deliver_rows)

    def pushed_group(i):
        group_copy(i, push_v, send2_sem, recv2_sem).wait_recv()

    def deliver_pair(p):
        deliver(p * PAIR, lambda q: gt_s[g, group_at(p * PAIR + q, -1)])

    def deliver_group(p):
        loop(p * PAIR, p * PAIR + PAIR, pushed_group)
        deliver_pair(p)

    loop(0, N_BLK - 1, lambda i: loop_copy(i, push_v, send2_sem, recv2_sem).wait_recv())
    loop(0, LOOP_PAIRS, lambda p: deliver(N_GRP + p * PAIR, lambda q: lt_s[b, loop_at(p * PAIR + q, -1)]))
    loop(Y_LINE, N_GRP, pushed_group)
    deliver_pair(GROUP_PAIRS - 1)
    loop(0, SELF // PAIR, deliver_group)
    pushed_group(SELF - 1)
    deliver_pair(SELF // PAIR)
    loop(N_Z // PAIR, GROUP_PAIRS - 2, deliver_group)
    pushed_group(Y_LINE - 1)
    deliver_pair(GROUP_PAIRS - 2)

    def sent_group(i):
        group_copy(i, push_v, send2_sem, recv2_sem).wait_send()

    loop(0, SELF, sent_group)
    loop(N_Z, N_GRP, sent_group)
    loop(0, N_BLK - 1, lambda i: loop_copy(i, push_v, send2_sem, recv2_sem).wait_send())


def put_out(out_v, box_v, out_h, box_h, sem):
    copies = [pltpu.make_async_copy(out_v, out_h, sem.at[0]), pltpu.make_async_copy(box_v, box_h, sem.at[1])]
    for copy in copies:
        copy.start()
    for copy in copies:
        copy.wait()


def body(features, initial, history, weight, column_ids, block_values, group_table, loop_table):
    f32, bf16, i32 = jnp.float32, jnp.bfloat16, jnp.int32
    blocks = (TILES, EDGE, HIDDEN)
    any_space, vmem = pl.BlockSpec(memory_space=pl.ANY), pl.BlockSpec(memory_space=pltpu.VMEM)
    dma = pltpu.SemaphoreType.DMA
    far = (N_FAR, EDGE, HIDDEN)
    refreshed, inbox = pl.pallas_call(
        kernel,
        out_shape=[pltpu.VMEM(blocks, f32)] * 2,
        in_specs=[any_space] * 8,
        out_specs=[vmem, vmem],
        scratch_shapes=[
            pltpu.VMEM(blocks, bf16),
            pltpu.VMEM(blocks, bf16),
            pltpu.VMEM((HIDDEN, HIDDEN), bf16),
            pltpu.VMEM((TILES, ENTRIES), i32),
            pltpu.VMEM(blocks, bf16),
            pltpu.VMEM((NONE + 1, EDGE, EDGE), bf16),
            pltpu.VMEM((NONE + 1, EDGE, EDGE), bf16),
            pltpu.VMEM((ENTRIES + 1, EDGE, EDGE), f32),
            pltpu.VMEM((GROUP_PAIRS, ROWS, 2 * PAIR * EDGE), bf16),
            pltpu.VMEM(far, bf16),
            pltpu.VMEM(far, bf16),
            pltpu.VMEM(far, bf16),
            pltpu.VMEM((ROWS, HIDDEN), bf16),
            pltpu.VMEM((16, 128), i32),
            pltpu.VMEM((16, 128), i32),
            pltpu.SMEM((16, 128), i32),
            pltpu.SMEM((16, 128), i32),
            pltpu.SMEM((N_GRP, N_GRP), i32),
            pltpu.SMEM((N_BLK, N_BLK), i32),
            dma((8,)),
            dma((2,)),
            pltpu.SemaphoreType.REGULAR,
            dma((N_FAR,)),
            dma((N_FAR,)),
            dma((N_FAR,)),
            dma((N_FAR,)),
        ],
        compiler_params=pltpu.CompilerParams(
            collective_id=0, has_side_effects=True, vmem_limit_bytes=60 * 2**20
        ),
    )(
        features.reshape(blocks),
        initial.reshape(blocks),
        history.reshape(blocks),
        weight,
        column_ids,
        block_values.reshape(NONE, EDGE, EDGE),
        group_table[0],
        loop_table[0],
    )
    held = [pltpu.with_memory_space_constraint(array, pltpu.VMEM) for array in (refreshed, inbox)]
    refreshed, inbox = pl.pallas_call(
        put_out,
        out_shape=[jax.ShapeDtypeStruct(blocks, f32)] * 2,
        in_specs=[vmem] * 2,
        out_specs=[any_space] * 2,
        scratch_shapes=[dma((2,))],
        compiler_params=pltpu.CompilerParams(vmem_limit_bytes=4 * 2**20),
    )(*held)
    return refreshed.reshape(ROWS, HIDDEN), inbox.reshape(ROWS, HIDDEN)


def solution(mesh):
    in_specs = (
        P(("blk", "grp"), None),
        P(("blk", "grp"), None),
        P(("blk", "grp"), None),
        P(),
        P(("blk", "grp"), None),
        P(("blk", "grp"), None, None, None),
        P("blk", None, None),
        P("grp", None, None),
    )
    out_specs = (P(("blk", "grp"), None), P(("blk", "grp"), None))
    return jax.shard_map(body, mesh=mesh, in_specs=in_specs, out_specs=out_specs, check_vma=False)
```

```python
import jax
import jax.numpy as jnp
from jax import lax
from jax.experimental import pallas as pl
from jax.experimental.pallas import tpu as pltpu
from jax.sharding import PartitionSpec as P

MESH = pl.DeviceIdType.MESH
teleport = 0.1
mapping_share = 0.5

TILES, ENTRIES, EDGE, HIDDEN = 12, 16, 128, 256
N_Z, N_Y, N_X, N_CORE = 8, 4, 4, 2
N_GRP, N_BLK = N_Z * N_Y, N_X * N_CORE
N_FAR = N_GRP + N_BLK
SELF = N_Z - 1
Y_LINE = N_GRP - (N_Y - 1)
PAIR = 2
OWN_PAIRS, LOOP_PAIRS, GROUP_PAIRS = TILES // PAIR, N_BLK // PAIR, N_GRP // PAIR
BAND = 6
ROWS = TILES * EDGE
NONE = TILES * ENTRIES


def far_first(k, n):
    return lax.rem(n // 2 + (1 - 2 * lax.rem(k, 2)) * lax.div(k + 1, 2) + n, n)


def kernel(
    feat_h, init_h, hist_h, w_h, ids_h, val_h, gt_h, lt_h,
    out_v, box_v,
    hist_v, init_v, w_v, ids_v, own_v, val_v, low_v, chain_v, adj_v, send_v, pull_v, push_v,
    left_v, last_v, prev_v, last_s, prev_s, gt_s, lt_s,
    in_sem, tab_sem, line_sem, send_sem, recv_sem, send2_sem, recv2_sem,
):
    f32, bf16 = jnp.float32, jnp.bfloat16
    g, b = lax.axis_index("grp"), lax.axis_index("blk")
    z, y = lax.div(g, N_Y), lax.rem(g, N_Y)
    x, core = lax.div(b, N_CORE), lax.rem(b, N_CORE)
    gath_v = box_v

    def group_of(dz, dy, sign):
        return lax.rem(z + sign * dz + N_Z, N_Z) * N_Y + lax.rem(y + sign * dy + N_Y, N_Y)

    def group_at(i, sign):
        r = jnp.maximum(i - N_Z, 0)
        on_z, on_y = i < N_Z, i >= Y_LINE
        dz = jnp.where(on_z, far_first(i, N_Z), jnp.where(on_y, 0, far_first(lax.div(r, N_Y - 1), N_Z)))
        dy = jnp.where(on_z, 0, far_first(lax.rem(r, N_Y - 1), N_Y))
        return group_of(dz, dy, sign)

    def loop_at(i, sign):
        dx, dc = far_first(lax.div(i, N_CORE), N_X), 1 - lax.rem(i, N_CORE)
        return lax.rem(x + sign * dx + N_X, N_X) * N_CORE + lax.rem(core + dc, N_CORE)

    def loop(lo, hi, body, unroll=1):
        def step(i, carry):
            for u in range(unroll):
                body(lo + i * unroll + u)
            return carry

        lax.fori_loop(0, (hi - lo) // unroll, step, 0)

    def group_copy(i, landing, ss, rs):
        return pltpu.make_async_remote_copy(
            src_ref=send_v.at[i], dst_ref=landing.at[i], send_sem=ss.at[i], recv_sem=rs.at[i],
            device_id={"grp": group_at(i, 1)}, device_id_type=MESH,
        )

    def loop_copy(i, landing, ss, rs):
        return pltpu.make_async_remote_copy(
            src_ref=send_v.at[N_GRP + i], dst_ref=landing.at[N_GRP + i],
            send_sem=ss.at[N_GRP + i], recv_sem=rs.at[N_GRP + i],
            device_id={"blk": loop_at(i, 1)}, device_id_type=MESH,
        )

    fetch_hist = pltpu.make_async_copy(hist_h, hist_v, in_sem.at[0])
    fetch_gt = pltpu.make_async_copy(gt_h, gt_s, in_sem.at[1])
    fetch_lt = pltpu.make_async_copy(lt_h, lt_s, in_sem.at[2])
    fetch_ids = pltpu.make_async_copy(ids_h, ids_v, in_sem.at[3])
    fetch_val = pltpu.make_async_copy(val_h, val_v.at[pl.ds(0, NONE)], in_sem.at[4])
    fetch_feat = pltpu.make_async_copy(feat_h, out_v, in_sem.at[5])
    fetch_init = pltpu.make_async_copy(init_h, init_v, in_sem.at[6])
    fetch_w = pltpu.make_async_copy(w_h, w_v, in_sem.at[7])
    for fetch in (fetch_gt, fetch_lt, fetch_hist, fetch_ids):
        fetch.start()
    barrier = pltpu.get_barrier_semaphore()

    def greet_group(i):
        pl.semaphore_signal(barrier, inc=1, device_id={"grp": group_at(i, 1)}, device_id_type=MESH)

    def greet_loop(i):
        pl.semaphore_signal(barrier, inc=1, device_id={"blk": loop_at(i, 1)}, device_id_type=MESH)

    loop(0, SELF, greet_group)
    loop(Y_LINE, N_GRP, greet_group)
    loop(0, N_BLK - 1, greet_loop)
    for fetch in (fetch_val, fetch_feat, fetch_init, fetch_w):
        fetch.start()

    fetch_gt.wait()
    fetch_lt.wait()
    fetch_hist.wait()

    def stage_group(i):
        send_v[i] = hist_v[gt_s[g, group_at(i, 1)]]

    def stage_loop(i):
        send_v[N_GRP + i] = hist_v[lt_s[b, loop_at(i, 1)]]

    loop(0, SELF, stage_group)
    loop(SELF + 1, N_GRP, stage_group)
    loop(0, N_BLK - 1, stage_loop)
    pull_v[SELF] = hist_v[gt_s[g, g]]
    pull_v[N_FAR - 1] = hist_v[lt_s[b, b]]

    def pull_group(i):
        group_copy(i, pull_v, send_sem, recv_sem).start()

    pl.semaphore_wait(barrier, (N_Z - 1) + (N_Y - 1) + (N_BLK - 1))

    def greet_line(i):
        pl.semaphore_signal(line_sem, inc=1, device_id={"grp": group_at(i, 1)}, device_id_type=MESH)

    loop(Y_LINE, N_GRP, greet_line)
    loop(0, SELF, pull_group)
    loop(Y_LINE, N_GRP, pull_group)
    loop(0, N_BLK - 1, lambda i: loop_copy(i, pull_v, send_sem, recv_sem).start())
    pl.semaphore_wait(line_sem, N_Y - 1)
    loop(N_Z, Y_LINE, pull_group)

    fetch_ids.wait()
    ids = ids_v[...]
    wide = (TILES, 128)
    tile = lax.broadcasted_iota(jnp.int32, wide, 0)
    slot = lax.broadcasted_iota(jnp.int32, wide, 1)
    entry = lax.broadcasted_iota(jnp.int32, ids.shape, 1)
    last = jnp.full(wide, NONE, jnp.int32)
    prev = jnp.full(ids.shape, ENTRIES, jnp.int32)
    for k in range(ENTRIES):
        column = ids[:, k : k + 1]
        last = jnp.where(column == slot, tile * ENTRIES + k, last)
        prev = jnp.where(jnp.logical_and(column == ids, entry > k), k, prev)
    last_v[...] = jnp.zeros_like(last_v)
    prev_v[...] = jnp.zeros_like(prev_v)
    last_v[pl.ds(0, TILES), :] = last
    prev_v[pl.ds(0, TILES), pl.ds(0, ENTRIES)] = prev
    put_last = pltpu.make_async_copy(last_v, last_s, tab_sem.at[0])
    put_prev = pltpu.make_async_copy(prev_v, prev_s, tab_sem.at[1])
    put_last.start()
    put_prev.start()
    put_last.wait()
    put_prev.wait()

    fetch_val.wait()
    for none in (val_v, low_v):
        none[NONE] = jnp.zeros((EDGE, EDGE), bf16)
    chain_v[ENTRIES] = jnp.zeros((EDGE, EDGE), f32)

    def chain_tile(t):
        def chain_entry(k):
            e = t * ENTRIES + k
            total = val_v[e].astype(f32) + chain_v[prev_s[t, k]]
            high = total.astype(bf16)
            chain_v[k] = total
            val_v[e] = high
            low_v[e] = (total - high.astype(f32)).astype(bf16)

        loop(0, ENTRIES, chain_entry, 4)

    loop(0, TILES, chain_tile)

    def group_slot(i, sign):
        return TILES + group_at(i, sign)

    def loop_slot(i, sign):
        return TILES + N_GRP + loop_at(i, sign)

    def lay_out(pair, first, second):
        def lay_tile(t):
            rows = pl.ds(pl.multiple_of(t * EDGE, EDGE), EDGE)
            for q, c in enumerate((first, second)):
                e = last_s[t, c]
                adj_v[pair, rows, pl.ds(q * EDGE, EDGE)] = val_v[e]
                adj_v[pair, rows, pl.ds((PAIR + q) * EDGE, EDGE)] = low_v[e]

        loop(0, TILES, lay_tile, 4)

    fetch_feat.wait()

    def own_block(t):
        own_v[t] = out_v[t].astype(bf16)
        gath_v[t] = jnp.zeros((EDGE, HIDDEN), f32)

    loop(0, TILES, own_block)

    def product_of(pair, blocks_ref, first, m):
        right = blocks_ref[pl.ds(first, PAIR)].reshape(PAIR * EDGE, HIDDEN)
        right = jnp.concatenate([right, right], axis=0)
        rows = pl.ds(pl.multiple_of(m * BAND * EDGE, BAND * EDGE), BAND * EDGE)
        part = jnp.dot(adj_v[pair, rows, :], right, preferred_element_type=f32)
        return part.reshape(BAND, EDGE, HIDDEN)

    def gather(pair, blocks_ref, first, pairs=1):
        def gather_rows(m):
            part = product_of(pair, blocks_ref, first, m)
            for extra in range(1, pairs):
                part = part + product_of(pair + extra, blocks_ref, first + extra * PAIR, m)
            gath_v[pl.ds(m * BAND, BAND)] += part

        loop(0, TILES // BAND, gather_rows)

    loop(0, OWN_PAIRS, lambda p: lay_out(p, p * PAIR, p * PAIR + 1))
    loop(0, OWN_PAIRS // 2, lambda p: gather(2 * p, own_v, 2 * p * PAIR, 2))
    loop(0, N_BLK - 1, lambda i: loop_copy(i, pull_v, send_sem, recv_sem).wait_recv())

    loop(0, LOOP_PAIRS, lambda p: lay_out(p, loop_slot(p * PAIR, -1), loop_slot(p * PAIR + 1, -1)))
    loop(0, LOOP_PAIRS // 2, lambda p: gather(2 * p, pull_v, N_GRP + 2 * p * PAIR, 2))
    loop(0, GROUP_PAIRS, lambda p: lay_out(p, group_slot(p * PAIR, -1), group_slot(p * PAIR + 1, -1)))
    fetch_init.wait()
    fetch_w.wait()

    def pulled_group(i):
        group_copy(i, pull_v, send_sem, recv_sem).wait_recv()

    def gather_group(p):
        loop(2 * p * PAIR, 2 * p * PAIR + 2 * PAIR, pulled_group)
        gather(2 * p, pull_v, 2 * p * PAIR, 2)

    loop(Y_LINE, N_GRP, pulled_group)
    gather(GROUP_PAIRS - 1, pull_v, N_GRP - PAIR)
    gather_group(0)
    loop(SELF - 3, SELF, pulled_group)
    gather(SELF // PAIR - 1, pull_v, SELF - 3, 2)
    loop(2, GROUP_PAIRS // 2 - 1, gather_group)
    pulled_group(Y_LINE - 1)

    def layer(m):
        gathered = gath_v[pl.ds(m * BAND, BAND)] + product_of(GROUP_PAIRS - 2, pull_v, Y_LINE - 1, m)
        start = init_v[pl.ds(m * BAND, BAND)].astype(f32)
        mixed = ((1.0 - teleport) * gathered + teleport * start).astype(bf16)
        mixed = mixed.reshape(BAND * EDGE, HIDDEN)
        product = jnp.dot(mixed, w_v[...], preferred_element_type=f32)
        fresh = jnp.maximum((1.0 - mapping_share) * mixed.astype(f32) + mapping_share * product, 0.0)
        out_v[pl.ds(m * BAND, BAND)] = fresh.reshape(BAND, EDGE, HIDDEN)
        left_v[pl.ds(pl.multiple_of(m * BAND * EDGE, BAND * EDGE), BAND * EDGE), :] = fresh.astype(bf16)

    loop(0, TILES // BAND, layer, 2)

    def message(c):
        left = jnp.concatenate([val_v[last_s[t, c]] for t in range(TILES)], axis=0)
        total = lax.dot_general(left, left_v[...], (((0,), (0,)), ((), ())), preferred_element_type=f32)
        return total.astype(bf16)

    def send_group(i):
        group_copy(i, pull_v, send_sem, recv_sem).wait_send()
        send_v[i] = message(group_slot(i, 1))
        group_copy(i, push_v, send2_sem, recv2_sem).start()

    def send_loop(i):
        loop_copy(i, pull_v, send_sem, recv_sem).wait_send()
        send_v[N_GRP + i] = message(loop_slot(i, 1))
        loop_copy(i, push_v, send2_sem, recv2_sem).start()

    loop(N_Z, Y_LINE, send_group)
    loop(0, SELF, send_group)
    loop(Y_LINE, N_GRP, send_group)
    loop(0, N_BLK - 1, send_loop)
    push_v[SELF] = message(TILES + g)
    push_v[N_FAR - 1] = message(TILES + N_GRP + b)

    def clear(t):
        box_v[t] = jnp.zeros((EDGE, HIDDEN), f32)

    loop(0, TILES, clear)

    def deliver(first, owner_block):
        owners = [owner_block(q) for q in range(PAIR)]

        def deliver_rows(r):
            rows = pl.ds(pl.multiple_of(r * 16, 16), 16)
            parts = [push_v[first + q, rows, :].astype(f32) for q in range(PAIR)]
            for t in range(TILES):
                total = box_v[t, rows, :]
                for q in range(PAIR):
                    total = total + jnp.where(owners[q] == t, parts[q], 0.0)
                box_v[t, rows, :] = total

        loop(0, EDGE // 16, deliver_rows)

    def pushed_group(i):
        group_copy(i, push_v, send2_sem, recv2_sem).wait_recv()

    def deliver_pair(p):
        deliver(p * PAIR, lambda q: gt_s[g, group_at(p * PAIR + q, -1)])

    def deliver_group(p):
        loop(p * PAIR, p * PAIR + PAIR, pushed_group)
        deliver_pair(p)

    loop(0, N_BLK - 1, lambda i: loop_copy(i, push_v, send2_sem, recv2_sem).wait_recv())
    loop(0, LOOP_PAIRS, lambda p: deliver(N_GRP + p * PAIR, lambda q: lt_s[b, loop_at(p * PAIR + q, -1)]))
    loop(N_Z // PAIR, GROUP_PAIRS - 2, deliver_group)
    loop(Y_LINE - 1, N_GRP, pushed_group)
    deliver_pair(GROUP_PAIRS - 2)
    deliver_pair(GROUP_PAIRS - 1)
    loop(0, SELF // PAIR, deliver_group)
    pushed_group(SELF - 1)
    deliver_pair(SELF // PAIR)

    def sent_group(i):
        group_copy(i, push_v, send2_sem, recv2_sem).wait_send()

    loop(0, SELF, sent_group)
    loop(N_Z, N_GRP, sent_group)
    loop(0, N_BLK - 1, lambda i: loop_copy(i, push_v, send2_sem, recv2_sem).wait_send())


def put_out(out_v, box_v, out_h, box_h, sem):
    copies = [pltpu.make_async_copy(out_v, out_h, sem.at[0]), pltpu.make_async_copy(box_v, box_h, sem.at[1])]
    for copy in copies:
        copy.start()
    for copy in copies:
        copy.wait()


def body(features, initial, history, weight, column_ids, block_values, group_table, loop_table):
    f32, bf16, i32 = jnp.float32, jnp.bfloat16, jnp.int32
    blocks = (TILES, EDGE, HIDDEN)
    any_space, vmem = pl.BlockSpec(memory_space=pl.ANY), pl.BlockSpec(memory_space=pltpu.VMEM)
    dma = pltpu.SemaphoreType.DMA
    far = (N_FAR, EDGE, HIDDEN)
    refreshed, inbox = pl.pallas_call(
        kernel,
        out_shape=[pltpu.VMEM(blocks, f32)] * 2,
        in_specs=[any_space] * 8,
        out_specs=[vmem, vmem],
        scratch_shapes=[
            pltpu.VMEM(blocks, bf16),
            pltpu.VMEM(blocks, bf16),
            pltpu.VMEM((HIDDEN, HIDDEN), bf16),
            pltpu.VMEM((TILES, ENTRIES), i32),
            pltpu.VMEM(blocks, bf16),
            pltpu.VMEM((NONE + 1, EDGE, EDGE), bf16),
            pltpu.VMEM((NONE + 1, EDGE, EDGE), bf16),
            pltpu.VMEM((ENTRIES + 1, EDGE, EDGE), f32),
            pltpu.VMEM((GROUP_PAIRS, ROWS, 2 * PAIR * EDGE), bf16),
            pltpu.VMEM(far, bf16),
            pltpu.VMEM(far, bf16),
            pltpu.VMEM(far, bf16),
            pltpu.VMEM((ROWS, HIDDEN), bf16),
            pltpu.VMEM((16, 128), i32),
            pltpu.VMEM((16, 128), i32),
            pltpu.SMEM((16, 128), i32),
            pltpu.SMEM((16, 128), i32),
            pltpu.SMEM((N_GRP, N_GRP), i32),
            pltpu.SMEM((N_BLK, N_BLK), i32),
            dma((8,)),
            dma((2,)),
            pltpu.SemaphoreType.REGULAR,
            dma((N_FAR,)),
            dma((N_FAR,)),
            dma((N_FAR,)),
            dma((N_FAR,)),
        ],
        compiler_params=pltpu.CompilerParams(
            collective_id=0, has_side_effects=True, vmem_limit_bytes=60 * 2**20
        ),
    )(
        features.reshape(blocks),
        initial.reshape(blocks),
        history.reshape(blocks),
        weight,
        column_ids,
        block_values.reshape(NONE, EDGE, EDGE),
        group_table[0],
        loop_table[0],
    )
    held = [pltpu.with_memory_space_constraint(array, pltpu.VMEM) for array in (refreshed, inbox)]
    refreshed, inbox = pl.pallas_call(
        put_out,
        out_shape=[jax.ShapeDtypeStruct(blocks, f32)] * 2,
        in_specs=[vmem] * 2,
        out_specs=[any_space] * 2,
        scratch_shapes=[dma((2,))],
        compiler_params=pltpu.CompilerParams(vmem_limit_bytes=4 * 2**20),
    )(*held)
    return refreshed.reshape(ROWS, HIDDEN), inbox.reshape(ROWS, HIDDEN)


def solution(mesh):
    in_specs = (
        P(("blk", "grp"), None),
        P(("blk", "grp"), None),
        P(("blk", "grp"), None),
        P(),
        P(("blk", "grp"), None),
        P(("blk", "grp"), None, None, None),
        P("blk", None, None),
        P("grp", None, None),
    )
    out_specs = (P(("blk", "grp"), None), P(("blk", "grp"), None))
    return jax.shard_map(body, mesh=mesh, in_specs=in_specs, out_specs=out_specs, check_vma=False)
```

```python
import jax
import jax.numpy as jnp
from jax import lax
from jax.experimental import pallas as pl
from jax.experimental.pallas import tpu as pltpu
from jax.sharding import PartitionSpec as P

MESH = pl.DeviceIdType.MESH
teleport = 0.1
mapping_share = 0.5

TILES, ENTRIES, EDGE, HIDDEN = 12, 16, 128, 256
N_Z, N_Y, N_X, N_CORE = 8, 4, 4, 2
N_GRP, N_BLK = N_Z * N_Y, N_X * N_CORE
N_FAR = N_GRP + N_BLK
SELF = N_Z - 1
Y_LINE = N_GRP - (N_Y - 1)
Z_FAR = 3
PAIR = 2
OWN_PAIRS, LOOP_PAIRS, GROUP_PAIRS = TILES // PAIR, N_BLK // PAIR, N_GRP // PAIR
BAND = 6
ROWS = TILES * EDGE
NONE = TILES * ENTRIES


def far_first(k, n):
    return lax.rem(n // 2 + (1 - 2 * lax.rem(k, 2)) * lax.div(k + 1, 2) + n, n)


def kernel(
    feat_h, init_h, hist_h, w_h, ids_h, val_h, gt_h, lt_h,
    out_v, box_v,
    hist_v, init_v, w_v, ids_v, own_v, val_v, low_v, chain_v, adj_v, send_v, pull_v, push_v,
    left_v, last_v, prev_v, last_s, prev_s, gt_s, lt_s,
    in_sem, tab_sem, line_sem, send_sem, recv_sem, send2_sem, recv2_sem,
):
    f32, bf16 = jnp.float32, jnp.bfloat16
    g, b = lax.axis_index("grp"), lax.axis_index("blk")
    z, y = lax.div(g, N_Y), lax.rem(g, N_Y)
    x, core = lax.div(b, N_CORE), lax.rem(b, N_CORE)
    gath_v = box_v

    def group_of(dz, dy, sign):
        return lax.rem(z + sign * dz + N_Z, N_Z) * N_Y + lax.rem(y + sign * dy + N_Y, N_Y)

    def group_at(i, sign):
        r = jnp.maximum(i - N_Z, 0)
        on_z, on_y = i < N_Z, i >= Y_LINE
        dz = jnp.where(on_z, far_first(i, N_Z), jnp.where(on_y, 0, far_first(lax.div(r, N_Y - 1), N_Z)))
        dy = jnp.where(on_z, 0, far_first(lax.rem(r, N_Y - 1), N_Y))
        return group_of(dz, dy, sign)

    def loop_at(i, sign):
        dx, dc = far_first(lax.div(i, N_CORE), N_X), 1 - lax.rem(i, N_CORE)
        return lax.rem(x + sign * dx + N_X, N_X) * N_CORE + lax.rem(core + dc, N_CORE)

    def loop(lo, hi, body, unroll=1):
        def step(i, carry):
            for u in range(unroll):
                body(lo + i * unroll + u)
            return carry

        lax.fori_loop(0, (hi - lo) // unroll, step, 0)

    def group_copy(i, landing, ss, rs):
        return pltpu.make_async_remote_copy(
            src_ref=send_v.at[i], dst_ref=landing.at[i], send_sem=ss.at[i], recv_sem=rs.at[i],
            device_id={"grp": group_at(i, 1)}, device_id_type=MESH,
        )

    def loop_copy(i, landing, ss, rs):
        return pltpu.make_async_remote_copy(
            src_ref=send_v.at[N_GRP + i], dst_ref=landing.at[N_GRP + i],
            send_sem=ss.at[N_GRP + i], recv_sem=rs.at[N_GRP + i],
            device_id={"blk": loop_at(i, 1)}, device_id_type=MESH,
        )

    fetch_hist = pltpu.make_async_copy(hist_h, hist_v, in_sem.at[0])
    fetch_gt = pltpu.make_async_copy(gt_h, gt_s, in_sem.at[1])
    fetch_lt = pltpu.make_async_copy(lt_h, lt_s, in_sem.at[2])
    fetch_ids = pltpu.make_async_copy(ids_h, ids_v, in_sem.at[3])
    fetch_val = pltpu.make_async_copy(val_h, val_v.at[pl.ds(0, NONE)], in_sem.at[4])
    fetch_feat = pltpu.make_async_copy(feat_h, out_v, in_sem.at[5])
    fetch_init = pltpu.make_async_copy(init_h, init_v, in_sem.at[6])
    fetch_w = pltpu.make_async_copy(w_h, w_v, in_sem.at[7])
    for fetch in (fetch_gt, fetch_lt, fetch_hist, fetch_ids):
        fetch.start()
    barrier = pltpu.get_barrier_semaphore()

    def greet_group(i):
        pl.semaphore_signal(barrier, inc=1, device_id={"grp": group_at(i, 1)}, device_id_type=MESH)

    def greet_loop(i):
        pl.semaphore_signal(barrier, inc=1, device_id={"blk": loop_at(i, 1)}, device_id_type=MESH)

    loop(0, SELF, greet_group)
    loop(Y_LINE, N_GRP, greet_group)
    loop(0, N_BLK - 1, greet_loop)
    for fetch in (fetch_val, fetch_feat, fetch_init, fetch_w):
        fetch.start()

    fetch_gt.wait()
    fetch_lt.wait()
    fetch_hist.wait()

    def stage_group(i):
        send_v[i] = hist_v[gt_s[g, group_at(i, 1)]]

    def stage_loop(i):
        send_v[N_GRP + i] = hist_v[lt_s[b, loop_at(i, 1)]]

    loop(0, SELF, stage_group)
    loop(SELF + 1, N_GRP, stage_group)
    loop(0, N_BLK - 1, stage_loop)
    pull_v[SELF] = hist_v[gt_s[g, g]]
    pull_v[N_FAR - 1] = hist_v[lt_s[b, b]]

    def pull_group(i):
        group_copy(i, pull_v, send_sem, recv_sem).start()

    pl.semaphore_wait(barrier, (N_Z - 1) + (N_Y - 1) + (N_BLK - 1))

    def greet_line(i):
        pl.semaphore_signal(line_sem, inc=1, device_id={"grp": group_at(i, 1)}, device_id_type=MESH)

    loop(Y_LINE, N_GRP, greet_line)
    loop(0, Z_FAR, pull_group)
    loop(Y_LINE, N_GRP, pull_group)
    loop(0, N_BLK - 1, lambda i: loop_copy(i, pull_v, send_sem, recv_sem).start())
    pl.semaphore_wait(line_sem, N_Y - 1)
    loop(N_Z, Y_LINE, pull_group)
    loop(Z_FAR, SELF, pull_group)

    fetch_ids.wait()
    ids = ids_v[...]
    wide = (TILES, 128)
    tile = lax.broadcasted_iota(jnp.int32, wide, 0)
    slot = lax.broadcasted_iota(jnp.int32, wide, 1)
    entry = lax.broadcasted_iota(jnp.int32, ids.shape, 1)
    last = jnp.full(wide, NONE, jnp.int32)
    prev = jnp.full(ids.shape, ENTRIES, jnp.int32)
    for k in range(ENTRIES):
        column = ids[:, k : k + 1]
        last = jnp.where(column == slot, tile * ENTRIES + k, last)
        prev = jnp.where(jnp.logical_and(column == ids, entry > k), k, prev)
    last_v[...] = jnp.zeros_like(last_v)
    prev_v[...] = jnp.zeros_like(prev_v)
    last_v[pl.ds(0, TILES), :] = last
    prev_v[pl.ds(0, TILES), pl.ds(0, ENTRIES)] = prev
    put_last = pltpu.make_async_copy(last_v, last_s, tab_sem.at[0])
    put_prev = pltpu.make_async_copy(prev_v, prev_s, tab_sem.at[1])
    put_last.start()
    put_prev.start()
    put_last.wait()
    put_prev.wait()

    fetch_val.wait()
    for none in (val_v, low_v):
        none[NONE] = jnp.zeros((EDGE, EDGE), bf16)
    chain_v[ENTRIES] = jnp.zeros((EDGE, EDGE), f32)

    def chain_tile(t):
        def chain_entry(k):
            e = t * ENTRIES + k
            total = val_v[e].astype(f32) + chain_v[prev_s[t, k]]
            high = total.astype(bf16)
            chain_v[k] = total
            val_v[e] = high
            low_v[e] = (total - high.astype(f32)).astype(bf16)

        loop(0, ENTRIES, chain_entry, 4)

    loop(0, TILES, chain_tile)

    def group_slot(i, sign):
        return TILES + group_at(i, sign)

    def loop_slot(i, sign):
        return TILES + N_GRP + loop_at(i, sign)

    def lay_out(pair, first, second):
        def lay_tile(t):
            rows = pl.ds(pl.multiple_of(t * EDGE, EDGE), EDGE)
            for q, c in enumerate((first, second)):
                e = last_s[t, c]
                adj_v[pair, rows, pl.ds(q * EDGE, EDGE)] = val_v[e]
                adj_v[pair, rows, pl.ds((PAIR + q) * EDGE, EDGE)] = low_v[e]

        loop(0, TILES, lay_tile, 4)

    fetch_feat.wait()

    def own_block(t):
        own_v[t] = out_v[t].astype(bf16)
        gath_v[t] = jnp.zeros((EDGE, HIDDEN), f32)

    loop(0, TILES, own_block)

    def product_of(pair, blocks_ref, first, m):
        right = blocks_ref[pl.ds(first, PAIR)].reshape(PAIR * EDGE, HIDDEN)
        right = jnp.concatenate([right, right], axis=0)
        rows = pl.ds(pl.multiple_of(m * BAND * EDGE, BAND * EDGE), BAND * EDGE)
        part = jnp.dot(adj_v[pair, rows, :], right, preferred_element_type=f32)
        return part.reshape(BAND, EDGE, HIDDEN)

    def gather(pair, blocks_ref, first, pairs=1):
        def gather_rows(m):
            part = product_of(pair, blocks_ref, first, m)
            for extra in range(1, pairs):
                part = part + product_of(pair + extra, blocks_ref, first + extra * PAIR, m)
            gath_v[pl.ds(m * BAND, BAND)] += part

        loop(0, TILES // BAND, gather_rows)

    loop(0, OWN_PAIRS, lambda p: lay_out(p, p * PAIR, p * PAIR + 1))
    loop(0, OWN_PAIRS // 2, lambda p: gather(2 * p, own_v, 2 * p * PAIR, 2))
    loop(0, N_BLK - 1, lambda i: loop_copy(i, pull_v, send_sem, recv_sem).wait_recv())

    loop(0, LOOP_PAIRS, lambda p: lay_out(p, loop_slot(p * PAIR, -1), loop_slot(p * PAIR + 1, -1)))
    loop(0, LOOP_PAIRS // 2, lambda p: gather(2 * p, pull_v, N_GRP + 2 * p * PAIR, 2))
    loop(0, GROUP_PAIRS, lambda p: lay_out(p, group_slot(p * PAIR, -1), group_slot(p * PAIR + 1, -1)))
    fetch_init.wait()
    fetch_w.wait()

    def pulled_group(i):
        group_copy(i, pull_v, send_sem, recv_sem).wait_recv()

    def gather_group(p):
        loop(2 * p * PAIR, 2 * p * PAIR + 2 * PAIR, pulled_group)
        gather(2 * p, pull_v, 2 * p * PAIR, 2)

    loop(Y_LINE, N_GRP, pulled_group)
    gather(GROUP_PAIRS - 1, pull_v, N_GRP - PAIR)
    loop(2, GROUP_PAIRS // 2 - 1, gather_group)
    pulled_group(Y_LINE - 1)
    gather(GROUP_PAIRS - 2, pull_v, Y_LINE - 1)
    gather_group(0)
    loop(2 * PAIR, SELF - 1, pulled_group)
    gather(2, pull_v, 2 * PAIR)
    pulled_group(SELF - 1)

    def layer(m):
        gathered = gath_v[pl.ds(m * BAND, BAND)] + product_of(SELF // PAIR, pull_v, SELF - 1, m)
        start = init_v[pl.ds(m * BAND, BAND)].astype(f32)
        mixed = ((1.0 - teleport) * gathered + teleport * start).astype(bf16)
        mixed = mixed.reshape(BAND * EDGE, HIDDEN)
        product = jnp.dot(mixed, w_v[...], preferred_element_type=f32)
        fresh = jnp.maximum((1.0 - mapping_share) * mixed.astype(f32) + mapping_share * product, 0.0)
        out_v[pl.ds(m * BAND, BAND)] = fresh.reshape(BAND, EDGE, HIDDEN)
        left_v[pl.ds(pl.multiple_of(m * BAND * EDGE, BAND * EDGE), BAND * EDGE), :] = fresh.astype(bf16)

    loop(0, TILES // BAND, layer, 2)

    def message(c):
        left = jnp.concatenate([val_v[last_s[t, c]] for t in range(TILES)], axis=0)
        total = lax.dot_general(left, left_v[...], (((0,), (0,)), ((), ())), preferred_element_type=f32)
        return total.astype(bf16)

    def send_group(i):
        group_copy(i, pull_v, send_sem, recv_sem).wait_send()
        send_v[i] = message(group_slot(i, 1))
        group_copy(i, push_v, send2_sem, recv2_sem).start()

    def send_loop(i):
        loop_copy(i, pull_v, send_sem, recv_sem).wait_send()
        send_v[N_GRP + i] = message(loop_slot(i, 1))
        loop_copy(i, push_v, send2_sem, recv2_sem).start()

    loop(N_Z, Y_LINE, send_group)
    loop(0, SELF, send_group)
    loop(Y_LINE, N_GRP, send_group)
    loop(0, N_BLK - 1, send_loop)
    push_v[SELF] = message(TILES + g)
    push_v[N_FAR - 1] = message(TILES + N_GRP + b)

    def clear(t):
        box_v[t] = jnp.zeros((EDGE, HIDDEN), f32)

    loop(0, TILES, clear)

    def deliver(first, owner_block):
        owners = [owner_block(q) for q in range(PAIR)]

        def deliver_rows(r):
            rows = pl.ds(pl.multiple_of(r * 16, 16), 16)
            parts = [push_v[first + q, rows, :].astype(f32) for q in range(PAIR)]
            for t in range(TILES):
                total = box_v[t, rows, :]
                for q in range(PAIR):
                    total = total + jnp.where(owners[q] == t, parts[q], 0.0)
                box_v[t, rows, :] = total

        loop(0, EDGE // 16, deliver_rows)

    def pushed_group(i):
        group_copy(i, push_v, send2_sem, recv2_sem).wait_recv()

    def deliver_pair(p):
        deliver(p * PAIR, lambda q: gt_s[g, group_at(p * PAIR + q, -1)])

    def deliver_group(p):
        loop(p * PAIR, p * PAIR + PAIR, pushed_group)
        deliver_pair(p)

    loop(0, N_BLK - 1, lambda i: loop_copy(i, push_v, send2_sem, recv2_sem).wait_recv())
    loop(0, LOOP_PAIRS, lambda p: deliver(N_GRP + p * PAIR, lambda q: lt_s[b, loop_at(p * PAIR + q, -1)]))
    loop(N_Z // PAIR, GROUP_PAIRS - 2, deliver_group)
    loop(Y_LINE - 1, N_GRP, pushed_group)
    deliver_pair(GROUP_PAIRS - 2)
    deliver_pair(GROUP_PAIRS - 1)
    loop(0, SELF // PAIR, deliver_group)
    pushed_group(SELF - 1)
    deliver_pair(SELF // PAIR)

    def sent_group(i):
        group_copy(i, push_v, send2_sem, recv2_sem).wait_send()

    loop(0, SELF, sent_group)
    loop(N_Z, N_GRP, sent_group)
    loop(0, N_BLK - 1, lambda i: loop_copy(i, push_v, send2_sem, recv2_sem).wait_send())


def put_out(out_v, box_v, out_h, box_h, sem):
    copies = [pltpu.make_async_copy(out_v, out_h, sem.at[0]), pltpu.make_async_copy(box_v, box_h, sem.at[1])]
    for copy in copies:
        copy.start()
    for copy in copies:
        copy.wait()


def body(features, initial, history, weight, column_ids, block_values, group_table, loop_table):
    f32, bf16, i32 = jnp.float32, jnp.bfloat16, jnp.int32
    blocks = (TILES, EDGE, HIDDEN)
    any_space, vmem = pl.BlockSpec(memory_space=pl.ANY), pl.BlockSpec(memory_space=pltpu.VMEM)
    dma = pltpu.SemaphoreType.DMA
    far = (N_FAR, EDGE, HIDDEN)
    refreshed, inbox = pl.pallas_call(
        kernel,
        out_shape=[pltpu.VMEM(blocks, f32)] * 2,
        in_specs=[any_space] * 8,
        out_specs=[vmem, vmem],
        scratch_shapes=[
            pltpu.VMEM(blocks, bf16),
            pltpu.VMEM(blocks, bf16),
            pltpu.VMEM((HIDDEN, HIDDEN), bf16),
            pltpu.VMEM((TILES, ENTRIES), i32),
            pltpu.VMEM(blocks, bf16),
            pltpu.VMEM((NONE + 1, EDGE, EDGE), bf16),
            pltpu.VMEM((NONE + 1, EDGE, EDGE), bf16),
            pltpu.VMEM((ENTRIES + 1, EDGE, EDGE), f32),
            pltpu.VMEM((GROUP_PAIRS, ROWS, 2 * PAIR * EDGE), bf16),
            pltpu.VMEM(far, bf16),
            pltpu.VMEM(far, bf16),
            pltpu.VMEM(far, bf16),
            pltpu.VMEM((ROWS, HIDDEN), bf16),
            pltpu.VMEM((16, 128), i32),
            pltpu.VMEM((16, 128), i32),
            pltpu.SMEM((16, 128), i32),
            pltpu.SMEM((16, 128), i32),
            pltpu.SMEM((N_GRP, N_GRP), i32),
            pltpu.SMEM((N_BLK, N_BLK), i32),
            dma((8,)),
            dma((2,)),
            pltpu.SemaphoreType.REGULAR,
            dma((N_FAR,)),
            dma((N_FAR,)),
            dma((N_FAR,)),
            dma((N_FAR,)),
        ],
        compiler_params=pltpu.CompilerParams(
            collective_id=0, has_side_effects=True, vmem_limit_bytes=60 * 2**20
        ),
    )(
        features.reshape(blocks),
        initial.reshape(blocks),
        history.reshape(blocks),
        weight,
        column_ids,
        block_values.reshape(NONE, EDGE, EDGE),
        group_table[0],
        loop_table[0],
    )
    held = [pltpu.with_memory_space_constraint(array, pltpu.VMEM) for array in (refreshed, inbox)]
    refreshed, inbox = pl.pallas_call(
        put_out,
        out_shape=[jax.ShapeDtypeStruct(blocks, f32)] * 2,
        in_specs=[vmem] * 2,
        out_specs=[any_space] * 2,
        scratch_shapes=[dma((2,))],
        compiler_params=pltpu.CompilerParams(vmem_limit_bytes=4 * 2**20),
    )(*held)
    return refreshed.reshape(ROWS, HIDDEN), inbox.reshape(ROWS, HIDDEN)


def solution(mesh):
    in_specs = (
        P(("blk", "grp"), None),
        P(("blk", "grp"), None),
        P(("blk", "grp"), None),
        P(),
        P(("blk", "grp"), None),
        P(("blk", "grp"), None, None, None),
        P("blk", None, None),
        P("grp", None, None),
    )
    out_specs = (P(("blk", "grp"), None), P(("blk", "grp"), None))
    return jax.shard_map(body, mesh=mesh, in_specs=in_specs, out_specs=out_specs, check_vma=False)
```
